256 devices in a mesh: grp: 2 (over core), dom: 128 (over y, x, z).
Axes of the slice: x: 4, y: 4, z: 8, core: 2. Of those that a mesh axis runs over, the one named last changes fastest.
Arguments:
- node_latent: bfloat16 [262144, 128], P(('grp', 'dom')), may hold values from -6 to 6
- edge_latent: bfloat16 [1572864, 128], P(('grp', 'dom')), may hold values from -6 to 6
- mig_send: int32 [256, 256], P(('grp', 'dom')), may hold values from 0 to 1024, as said below
- mig_recv: int32 [262144], P(('grp', 'dom')), may hold values from 0 to 1279, as said below
- halo_send: int32 [256, 128], P(('grp', 'dom')), may hold values from 0 to 1024, as said below
- cross_send: int32 [256, 32], P(('grp', 'dom')), may hold values from 0 to 1024, as said below
- senders: int32 [1572864], P(('grp', 'dom')), may hold values from 0 to 1183, as said below
- receivers: int32 [1572864], P(('grp', 'dom')), may hold values from 0 to 1023
- edge_live: int32 [1572864], P(('grp', 'dom')), may hold values from 0 to 1, as said below
- edge_w1: bfloat16 [384, 128], replicated, may hold values from -0.3125 to 0.3125
- edge_b1: float32 [128], replicated, may hold values from -2 to 2
- edge_w2: bfloat16 [128, 128], replicated, may hold values from -0.5 to 0.5
- edge_b2: float32 [128], replicated, may hold values from -2 to 2
- edge_gain: float32 [128], replicated, may hold values from 0.25 to 1.75
- edge_bias: float32 [128], replicated, may hold values from -2 to 2
- node_w1: bfloat16 [256, 128], replicated, may hold values from -0.375 to 0.375
- node_b1: float32 [128], replicated, may hold values from -2 to 2
- node_w2: bfloat16 [128, 128], replicated, may hold values from -0.5 to 0.5
- node_b2: float32 [128], replicated, may hold values from -2 to 2
- node_gain: float32 [128], replicated, may hold values from 0.25 to 1.75
- node_bias: float32 [128], replicated, may hold values from -2 to 2
Outputs:
- node_out: bfloat16 [262144, 128], P(('grp', 'dom'))
- edge_out: bfloat16 [1572864, 128], P(('grp', 'dom'))
The draws below stay inside these ranges and needn't reach their ends.
Inputs may be any that keep to these rules, and one draw needn't show every extreme that they name: `mig_send`: per partition, slot k * 64 + c names an old local row moving to the partition at distance o_k, or 1024 for an empty slot; live slots of one distance come first, every old row is named at most once, and a partition sends to a partition exactly as many rows as it receives from it. Where the peer exists, 32 or more slots of a distance are live; slots toward missing partitions are empty; in every draw some partition of each region fills all its slots both ways. `mig_recv`: for each partition, 1024 distinct entries of its source table: old rows it did not send and live arrived slots, each exactly once. `halo_send`: slot k * 32 + c names a new local row sent to the partition at distance o_k, or 1024 if empty; live slots come first, rows are distinct within a partition; where the peer exists 32 // 2 or more are live, and some partition of each region fills all slots whose peer exists. `cross_send`: new local rows sent to the same partition of the other region, or 1024 if empty; live slots come first, 16 or more live, distinct from that partition's halo_send rows; some partition of each region fills all. `senders`: each entry names a new local row (below 1024) or a live halo or cross slot of the extended table. `edge_live`: within a partition, the live edge slots are a prefix of at least 3072 slots; some partition is fully live in every draw.
All inputs are finite; a program needn't handle non-finite values.
Results may differ from the reference program's by a relative error of at most 0.0075.
Values may be sent and summed in bfloat16 or wider, within the bound.
A program may use at most 64 MiB of HBM per device.

```python
import jax
import jax.numpy as jnp
from jax import lax

L = 128
R = 2
CAP = 64
HCAP = 32
XCAP = 32
TILE = 128
NODES_DEV = 1024
ETILES = 48
NODES = 262144
EDGES = 1572864
N_GRP = 2
N_DOM = 128


def offset_list_drawn():
    return [number - R if number < R else number - R + 1 for number in range(2 * R)]


def move_counts(counts, shift_by):
    domain = jnp.arange(N_DOM, dtype=jnp.int32) - shift_by
    inside = (domain >= 0) & (domain < N_DOM)
    return jnp.where(inside[None, :], counts[:, jnp.clip(domain, 0, N_DOM - 1)], 0)


def distinct_order(key, length):
    scores = jax.random.randint(key, (N_GRP, N_DOM, length), 0, 2 ** 14) * 32768 + jnp.arange(length, dtype=jnp.int32)
    return jnp.argsort(scores, axis=-1).astype(jnp.int32)


def layout_plan(key):
    groups = N_GRP
    parts = N_DOM
    distances = 2 * R
    shifts = offset_list_drawn()
    domain = jnp.arange(parts, dtype=jnp.int32)
    centre = jax.random.randint(jax.random.fold_in(key, 11), (groups,), R, parts - R)
    flows = jax.random.randint(jax.random.fold_in(key, 12), (groups, parts, R), CAP // 2, CAP + 1)
    reach = jnp.arange(1, R + 1, dtype=jnp.int32)
    touches = (domain[None, :, None] == centre[:, None, None]) | (domain[None, :, None] + reach[None, None, :] == centre[:, None, None])
    flows = jnp.where(touches, CAP, flows)
    flows = jnp.where(domain[None, :, None] + reach[None, None, :] < parts, flows, 0)
    columns = []
    for shift in shifts:
        if shift > 0:
            columns.append(flows[:, :, shift - 1])
        else:
            columns.append(move_counts(flows[:, :, -shift - 1], -shift))
    counts = jnp.stack(columns, axis=2)
    arrivals = jnp.stack([move_counts(counts[:, :, place], shift) for place, shift in enumerate(shifts)], axis=2)
    order = distinct_order(jax.random.fold_in(key, 13), NODES_DEV)
    starts = jnp.cumsum(counts, axis=2) - counts
    outgoing = jnp.sum(counts, axis=2)
    slot_ids = jnp.arange(CAP, dtype=jnp.int32)
    positions = jnp.minimum(starts[..., None] + slot_ids, NODES_DEV - 1).reshape(groups, parts, distances * CAP)
    chosen = jnp.take_along_axis(order, positions, axis=2).reshape(groups, parts, distances, CAP)
    mig_send = jnp.where(slot_ids < counts[..., None], chosen, NODES_DEV).reshape(groups * parts, distances * CAP)
    ranks = jnp.argsort(order, axis=-1).astype(jnp.int32)
    kept = ranks >= outgoing[..., None]
    landed = (slot_ids < arrivals[..., None]).reshape(groups, parts, distances * CAP)
    usable = jnp.concatenate([kept, landed], axis=2).astype(jnp.int32)
    table_len = NODES_DEV + distances * CAP
    scores = (1 - usable) * 2 ** 30 + jax.random.randint(jax.random.fold_in(key, 14), (groups, parts, table_len), 0, 2 ** 14) * 32768 + jnp.arange(table_len, dtype=jnp.int32)
    mig_recv = jnp.argsort(scores, axis=-1).astype(jnp.int32)[..., :NODES_DEV].reshape(-1)
    halo_centre = jax.random.randint(jax.random.fold_in(key, 15), (groups,), 0, parts)
    halo_counts = jax.random.randint(jax.random.fold_in(key, 16), (groups, parts, distances), HCAP // 2, HCAP + 1)
    halo_counts = jnp.where(domain[None, :, None] == halo_centre[:, None, None], HCAP, halo_counts)
    shift_arr = jnp.array(shifts, dtype=jnp.int32)
    target = domain[None, :, None] + shift_arr[None, None, :]
    halo_counts = jnp.where((target >= 0) & (target < parts), halo_counts, 0)
    second = distinct_order(jax.random.fold_in(key, 17), NODES_DEV)
    halo_ids = jnp.arange(HCAP, dtype=jnp.int32)
    halo_rows = second[..., :distances * HCAP].reshape(groups, parts, distances, HCAP)
    halo_send = jnp.where(halo_ids < halo_counts[..., None], halo_rows, NODES_DEV).reshape(groups * parts, distances * HCAP)
    cross_counts = jax.random.randint(jax.random.fold_in(key, 18), (groups, parts), XCAP // 2, XCAP + 1)
    cross_counts = jnp.where(domain[None, :] == halo_centre[:, None], XCAP, cross_counts)
    cross_ids = jnp.arange(XCAP, dtype=jnp.int32)
    cross_rows = second[..., distances * HCAP:distances * HCAP + XCAP]
    cross_send = jnp.where(cross_ids < cross_counts[..., None], cross_rows, NODES_DEV).reshape(groups * parts, XCAP)
    halo_arrivals = jnp.stack([move_counts(halo_counts[:, :, place], shift) for place, shift in enumerate(shifts)], axis=2)
    cross_arrivals = jnp.flip(cross_counts, axis=0)
    remote_live = jnp.concatenate([(halo_ids < halo_arrivals[..., None]).reshape(groups, parts, distances * HCAP), cross_ids < cross_arrivals[..., None]], axis=2).astype(jnp.int32)
    return (mig_send, mig_recv, halo_send, cross_send, remote_live)


def draw_mig_send(key, part):
    return layout_plan(key)[0]


def draw_mig_recv(key, part):
    return layout_plan(key)[1]


def draw_halo_send(key, part):
    return layout_plan(key)[2]


def draw_cross_send(key, part):
    return layout_plan(key)[3]


def draw_senders(key, part):
    remote_live = layout_plan(key)[4]
    remote_len = remote_live.shape[2]
    edges_dev = ETILES * TILE
    scores = (1 - remote_live) * 65536 + jnp.arange(remote_len, dtype=jnp.int32)
    remote_order = jnp.argsort(scores, axis=-1).astype(jnp.int32)
    live_total = jnp.sum(remote_live, axis=2)
    picks = jax.random.randint(jax.random.fold_in(key, 21), (N_GRP, N_DOM, edges_dev), 0, 2 ** 20) % live_total[..., None]
    remote = NODES_DEV + jnp.take_along_axis(remote_order, picks, axis=2)
    local = jax.random.randint(jax.random.fold_in(key, 22), (N_GRP, N_DOM, edges_dev), 0, NODES_DEV)
    faraway = jax.random.randint(jax.random.fold_in(key, 23), (N_GRP, N_DOM, edges_dev), 0, 10) < 3
    return jnp.where(faraway, remote, local).astype(jnp.int32).reshape(-1)


def draw_edge_live(key, part):
    edges_dev = ETILES * TILE
    counts = jax.random.randint(jax.random.fold_in(key, 31), (N_GRP * N_DOM,), edges_dev // 2, edges_dev + 1)
    fullest = jax.random.randint(jax.random.fold_in(key, 32), (), 0, N_GRP * N_DOM)
    counts = jnp.where(jnp.arange(N_GRP * N_DOM, dtype=jnp.int32) == fullest, edges_dev, counts)
    slots = jnp.arange(edges_dev, dtype=jnp.int32)
    return (slots[None, :] < counts[:, None]).astype(jnp.int32).reshape(-1)


def touch_ends(entries, key, smallest, largest):
    dims = entries.shape
    spot = [jax.random.randint(jax.random.fold_in(key, axis), (), 0, dims[axis]) for axis in range(len(dims))]
    entries = entries.at[tuple(spot)].set(smallest)
    longest = dims.index(max(dims))
    spot[longest] = (spot[longest] + 1) % dims[longest]
    return entries.at[tuple(spot)].set(largest)


def block_scale(own_key, dims, cuts, least, largest):
    loudness = 1.0
    for dim, shards_of in cuts:
        draws = jax.random.uniform(jax.random.fold_in(jax.random.fold_in(own_key, 6), dim), (shards_of,), jnp.float32, least / len(cuts), largest / len(cuts))
        loudness = loudness * jnp.repeat(jnp.exp(draws), dims[dim] // shards_of).reshape((-1,) + (1,) * (len(dims) - 1 - dim))
    return loudness


def centred(own_key, shape, deviation, bound, split=(), kind=jnp.bfloat16):
    loudness = block_scale(own_key, shape, split, -0.22, 0.18) if split else 1.0
    drawn = jax.random.normal(own_key, shape, jnp.float32) * deviation * loudness
    return jnp.minimum(jnp.maximum(drawn, -bound), bound).astype(kind)


def setup_inputs(seed: int = 0) -> dict:
    streams_of = jax.random.split(jax.random.key(seed), 22)
    return {
        "node_latent": centred(streams_of[0], (NODES, L), 1.0, 6.0, ((0, 256),)),
        "edge_latent": centred(streams_of[1], (EDGES, L), 1.0, 6.0, ((0, 256),)),
        "mig_send": draw_mig_send(jax.random.fold_in(streams_of[21], 71), 0),
        "mig_recv": draw_mig_recv(jax.random.fold_in(streams_of[21], 71), 0),
        "halo_send": draw_halo_send(jax.random.fold_in(streams_of[21], 71), 0),
        "cross_send": draw_cross_send(jax.random.fold_in(streams_of[21], 71), 0),
        "senders": draw_senders(jax.random.fold_in(streams_of[21], 71), 0),
        "receivers": touch_ends(jax.random.randint(streams_of[7], (EDGES,), 0, NODES_DEV), jax.random.fold_in(streams_of[7], 1), 0, NODES_DEV - 1).astype(jnp.int32),
        "edge_live": draw_edge_live(jax.random.fold_in(streams_of[21], 71), 0),
        "edge_w1": centred(streams_of[9], (3 * L, L), (3 * L) ** -0.5, 0.3125),
        "edge_b1": centred(streams_of[10], (L,), 0.3, 2.0, (), jnp.float32),
        "edge_w2": centred(streams_of[11], (L, L), L ** -0.5, 0.5),
        "edge_b2": centred(streams_of[12], (L,), 0.3, 2.0, (), jnp.float32),
        "edge_gain": jnp.clip(1.0 + 0.15 * jax.random.normal(streams_of[13], (L,), jnp.float32), 0.25, 1.75),
        "edge_bias": centred(streams_of[14], (L,), 0.3, 2.0, (), jnp.float32),
        "node_w1": centred(streams_of[15], (2 * L, L), (2 * L) ** -0.5, 0.375),
        "node_b1": centred(streams_of[16], (L,), 0.3, 2.0, (), jnp.float32),
        "node_w2": centred(streams_of[17], (L, L), L ** -0.5, 0.5),
        "node_b2": centred(streams_of[18], (L,), 0.3, 2.0, (), jnp.float32),
        "node_gain": jnp.clip(1.0 + 0.15 * jax.random.normal(streams_of[19], (L,), jnp.float32), 0.25, 1.75),
        "node_bias": centred(streams_of[20], (L,), 0.3, 2.0, (), jnp.float32),
    }


EPSILON = 1e-05

def offset_list():
    return [number - R if number < R else number - R + 1 for number in range(2 * R)]

def layer_norm(values, scale_vec, offset_vec):
    center = values - lax.optimization_barrier(jnp.mean(values, axis=-1, keepdims=True))
    spread = lax.optimization_barrier(jnp.mean(center * center, axis=-1, keepdims=True))
    return center * lax.rsqrt(spread + EPSILON) * scale_vec + offset_vec

def select_rows(source_rows, wanted):
    padded = jnp.concatenate([source_rows, jnp.zeros((1, source_rows.shape[1]), source_rows.dtype)], axis=0)
    return padded[jnp.minimum(wanted, source_rows.shape[0]).astype(jnp.int32)]

def move_along(stacked, shift_by):
    domain = jnp.arange(N_DOM, dtype=jnp.int32) - shift_by
    inside = (domain >= 0) & (domain < N_DOM)
    moved = stacked[:, jnp.clip(domain, 0, N_DOM - 1)]
    inside = inside.reshape((1, N_DOM) + (1,) * (stacked.ndim - 2))
    return jnp.where(inside, moved, jnp.zeros((), stacked.dtype))

def deliver(outgoing):
    return jnp.stack([move_along(outgoing[:, :, position], shift) for position, shift in enumerate(offset_list())], axis=2)

def reference(node_latent, edge_latent, mig_send, mig_recv, halo_send, cross_send, senders, receivers, edge_live, edge_w1, edge_b1, edge_w2, edge_b2, edge_gain, edge_bias, node_w1, node_b1, node_w2, node_b2, node_gain, node_bias):
    latent = node_latent.shape[1]
    groups = N_GRP
    parts = N_DOM
    per_device = jax.vmap(jax.vmap(select_rows))
    old_rows = node_latent.reshape(groups, parts, NODES_DEV, latent)
    leaving = per_device(old_rows, mig_send.reshape(groups, parts, 2 * R * CAP)).reshape(groups, parts, 2 * R, CAP, latent)
    arrived = deliver(leaving).reshape(groups, parts, 2 * R * CAP, latent)
    source_rows = jnp.concatenate([old_rows, arrived], axis=2)
    direct_take = jax.vmap(jax.vmap(lambda table_rows, wanted: table_rows[wanted]))
    fresh = direct_take(source_rows, mig_recv.reshape(groups, parts, NODES_DEV))
    halo_out = per_device(fresh, halo_send.reshape(groups, parts, 2 * R * HCAP)).reshape(groups, parts, 2 * R, HCAP, latent)
    halo_in = deliver(halo_out).reshape(groups, parts, 2 * R * HCAP, latent)
    cross_out = per_device(fresh, cross_send.reshape(groups, parts, XCAP))
    cross_in = jnp.flip(cross_out, axis=0)
    extended = jnp.concatenate([fresh, halo_in, cross_in], axis=2).reshape(groups * parts, -1, latent)
    fresh_flat = fresh.reshape(groups * parts, NODES_DEV, latent)
    edges_dev = ETILES * TILE
    wide = jnp.float32

    def device_layer(items):
        fresh_rows, extended_rows, edge_rows, sender_ids, receiver_ids, active = items
        sent_side = extended_rows[sender_ids]
        recv_side = fresh_rows[receiver_ids]
        joined = jnp.concatenate([edge_rows, sent_side, recv_side], axis=1).astype(wide)
        hidden = jnp.maximum(jnp.dot(joined, edge_w1.astype(wide)) + edge_b1, 0.0).astype(jnp.bfloat16)
        before = jnp.dot(hidden.astype(wide), edge_w2.astype(wide)) + edge_b2
        message = layer_norm(before, edge_gain, edge_bias).astype(jnp.bfloat16)
        kept = message.astype(wide) * active.astype(wide)[:, None]
        new_edges = (edge_rows.astype(wide) + kept).astype(jnp.bfloat16)
        inbound = jax.ops.segment_sum(kept, receiver_ids, num_segments=NODES_DEV).astype(jnp.bfloat16)
        node_in = jnp.concatenate([fresh_rows, inbound], axis=1).astype(wide)
        node_hidden = jnp.maximum(jnp.dot(node_in, node_w1.astype(wide)) + node_b1, 0.0).astype(jnp.bfloat16)
        node_before = jnp.dot(node_hidden.astype(wide), node_w2.astype(wide)) + node_b2
        new_nodes = (fresh_rows.astype(wide) + layer_norm(node_before, node_gain, node_bias)).astype(jnp.bfloat16)
        return (new_nodes, new_edges)
    new_nodes, new_edges = lax.map(device_layer, (fresh_flat, extended, edge_latent.reshape(groups * parts, edges_dev, latent), senders.reshape(groups * parts, edges_dev), receivers.reshape(groups * parts, edges_dev), edge_live.reshape(groups * parts, edges_dev)))
    return (new_nodes.reshape(-1, latent), new_edges.reshape(-1, latent))
```

```python
import functools

import jax
import jax.numpy as jnp
from jax import lax
from jax.experimental import pallas as pl
from jax.experimental.pallas import tpu as pltpu
from jax.sharding import PartitionSpec as P

R = 2
EPSILON = 1e-05
L = 128
TILE = 512
HALF = 512
MESH = pl.DeviceIdType.MESH
F32, BF16, I32, I16 = jnp.float32, jnp.bfloat16, jnp.int32, jnp.int16


def offset_list():
    return [number - R if number < R else number - R + 1 for number in range(2 * R)]


def dot(a, b):
    return jnp.dot(a, b, preferred_element_type=F32)


def down(row):
    return jnp.broadcast_to(row, (128, 128)).T


def one_hot(column, first, width):
    small = column.astype(I16)
    lanes = lax.broadcasted_iota(I32, (column.shape[0], 128), 1).astype(I16)
    pieces = []
    for start in range(0, width, 128):
        hit = (small - jnp.int16(first + start)) == lanes
        pieces.append(jnp.where(hit, jnp.bfloat16(1), jnp.bfloat16(0)))
    return jnp.concatenate(pieces, axis=1)


def layer_norm(values, gain, bias):
    center = values - jnp.mean(values, axis=-1, keepdims=True)
    spread = jnp.mean(center * center, axis=-1, keepdims=True)
    return center * lax.rsqrt(spread + EPSILON) * gain + bias


def exchange_kernel(count, old_ref, ms_ref, mr_ref, hs_ref, xs_ref, fresh_ref, halo_ref,
                    leave_buf, arrive_buf, out_buf, in_buf,
                    lsend, lrecv, hsend, hrecv):
    me = lax.axis_index("dom")
    other = 1 - lax.axis_index("grp")
    shifts = offset_list()
    peers = [lax.rem(me + shift + count, count) for shift in shifts]

    barrier = pltpu.get_barrier_semaphore()
    for peer in peers:
        pl.semaphore_signal(barrier, inc=1, device_id={"dom": peer}, device_id_type=MESH)
    pl.semaphore_signal(barrier, inc=1, device_id={"grp": other}, device_id_type=MESH)

    old = old_ref[...]
    nodes = old.shape[0]
    moves = ms_ref.shape[1] // len(shifts)
    halos = hs_ref.shape[1] // len(shifts)
    want = jnp.concatenate([down(ms_ref[:, i:i + 128]) for i in range(0, ms_ref.shape[1], 128)], axis=0)
    leave_buf[...] = dot(one_hot(want, 0, nodes), old).astype(BF16)
    pl.semaphore_wait(barrier, len(peers) + 1)

    copies = []
    for place, peer in enumerate(peers):
        rows = pl.ds(place * moves, moves)
        copy = pltpu.make_async_remote_copy(
            src_ref=leave_buf.at[rows], dst_ref=arrive_buf.at[rows],
            send_sem=lsend.at[place], recv_sem=lrecv.at[place],
            device_id={"dom": peer}, device_id_type=MESH)
        copy.start()
        copies.append(copy)

    take = jnp.concatenate([down(mr_ref[i:i + 1, :]) for i in range(mr_ref.shape[0])], axis=0)
    stay = dot(one_hot(take, 0, nodes), old)
    new = one_hot(take, nodes, arrive_buf.shape[0])
    hwant = jnp.concatenate([down(hs_ref[...]), down(xs_ref[...])[:32]], axis=0)
    hot = one_hot(hwant, 0, nodes)
    for copy in copies:
        copy.wait_recv()
    fresh = (stay + dot(new, arrive_buf[...])).astype(BF16)
    fresh_ref[...] = fresh
    out_buf[...] = dot(hot, fresh).astype(BF16)

    second = []
    for place, peer in enumerate(peers):
        rows = pl.ds(place * halos, halos)
        copy = pltpu.make_async_remote_copy(
            src_ref=out_buf.at[rows], dst_ref=in_buf.at[rows],
            send_sem=hsend.at[place], recv_sem=hrecv.at[place],
            device_id={"dom": peer}, device_id_type=MESH)
        copy.start()
        second.append(copy)
    rows = pl.ds(len(peers) * halos, 32)
    copy = pltpu.make_async_remote_copy(
        src_ref=out_buf.at[rows], dst_ref=in_buf.at[rows],
        send_sem=hsend.at[len(peers)], recv_sem=hrecv.at[len(peers)],
        device_id={"grp": other}, device_id_type=MESH)
    copy.start()
    second.append(copy)
    for copy in copies:
        copy.wait_send()
    for copy in second:
        copy.wait()
    halo_ref[...] = in_buf[...]


def layer_kernel(fresh_ref, halo_ref, snd_ref, rcv_ref, live_ref,
                 ew1_ref, eb1_ref, ew2_ref, eb2_ref, eg_ref, eo_ref,
                 nw1_ref, nb1_ref, nw2_ref, nb2_ref, ng_ref, no_ref, edge_hbm,
                 node_out, edge_out,
                 edge_buf, new_buf, send_tab, recv_tab, words, pre_buf, sums, in_sem, out_sem):
    edges = edge_buf.shape[0]
    tiles = edges // TILE
    subs = TILE // 128
    loads = [pltpu.make_async_copy(edge_hbm.at[pl.ds(i * TILE, TILE)], edge_buf.at[pl.ds(i * TILE, TILE)], in_sem.at[i])
             for i in range(tiles)]
    for load in loads:
        load.start()

    fresh = fresh_ref[...]
    halo = halo_ref[...]
    w1e, w1s, w1r = ew1_ref[0:L], ew1_ref[L:2 * L], ew1_ref[2 * L:3 * L]
    part = dot(fresh, w1s).astype(BF16)
    far = dot(halo, w1s).astype(BF16)
    send_tab[0:HALF, 0:L] = part[:HALF]
    send_tab[0:HALF, L:2 * L] = part[HALF:]
    send_tab[HALF:HALF + 128, 0:L] = far[:128]
    send_tab[HALF:HALF + 32, L:2 * L] = far[128:]
    send_tab[HALF + 32:HALF + 128, L:2 * L] = jnp.zeros((96, L), BF16)
    send_tab[HALF + 128:, 0:L] = w1e
    send_tab[HALF + 128:, L:2 * L] = w1e
    part = dot(fresh, w1r).astype(BF16)
    recv_tab[:, 0:L] = part[:HALF]
    recv_tab[:, L:2 * L] = part[HALF:]

    s, r, live = snd_ref[...], rcv_ref[...], live_ref[...]
    far_s = s >= 2 * HALF
    q = s - 2 * HALF
    s_row = jnp.where(far_s, HALF + (q & 127), s & (HALF - 1))
    s_half = jnp.where(far_s, q >> 7, s >> 9)
    r_row = r & (HALF - 1)
    r_half = r >> 9
    words[...] = s_row | (s_half << 10) | (r_row << 11) | (r_half << 21) | (live << 22)
    sums[...] = jnp.zeros_like(sums)

    w2 = ew2_ref[...]
    nil = jnp.zeros((L, L), BF16)
    w2_pair = jnp.concatenate([jnp.concatenate([w2, nil], axis=1), jnp.concatenate([nil, w2], axis=1)], axis=0)

    for tile in range(tiles):
        loads[tile].wait()
        spot = pl.ds(tile * TILE, TILE)
        word = jnp.concatenate([down(words[tile * subs + i:tile * subs + i + 1, :]) for i in range(subs)], axis=0)
        edge = edge_buf[spot]
        hot_s = jnp.concatenate([one_hot(word & 1023, 0, HALF + 128), edge], axis=1)
        got_s = dot(hot_s, send_tab[...])
        got_r = dot(one_hot((word >> 11) & 1023, 0, HALF), recv_tab[...])
        pre = (jnp.where((word & (1 << 10)) != 0, got_s[:, L:], got_s[:, :L])
               + jnp.where((word & (1 << 21)) != 0, got_r[:, L:], got_r[:, :L]))
        hidden = jnp.maximum(pre + eb1_ref[...], 0.0).astype(BF16)
        pair = jnp.concatenate([hidden[:TILE // 2], hidden[TILE // 2:]], axis=1)
        before = dot(pair, w2_pair)
        before = jnp.concatenate([before[:, :L], before[:, L:]], axis=0) + eb2_ref[...]
        message = layer_norm(before, eg_ref[...], eo_ref[...])
        kept = jnp.where((word & (1 << 22)) != 0, message, 0.0).astype(BF16)
        new_buf[spot] = (edge.astype(F32) + kept.astype(F32)).astype(BF16)
        pltpu.make_async_copy(new_buf.at[spot], edge_out.at[spot], out_sem.at[tile]).start()
        upper = ((word >> 11) & 1024).astype(I16) != jnp.int16(0)
        zero = jnp.zeros_like(kept)
        sides = jnp.concatenate([jnp.where(upper, zero, kept), jnp.where(upper, kept, zero)], axis=1)
        down_iota = lax.broadcasted_iota(I32, (HALF, 128), 0).astype(I16)
        flat = []
        for i in range(subs):
            row = (words[tile * subs + i:tile * subs + i + 1, :] >> 11) & 1023
            flat.append(jnp.where(jnp.broadcast_to(row, (HALF, 128)).astype(I16) == down_iota,
                                  jnp.bfloat16(1), jnp.bfloat16(0)))
        sums[...] += dot(jnp.concatenate(flat, axis=1), sides)

    inbound = jnp.concatenate([sums[:, :L], sums[:, L:]], axis=0).astype(BF16)
    node_in = jnp.concatenate([fresh, inbound], axis=1)
    node_hidden = jnp.maximum(dot(node_in, nw1_ref[...]) + nb1_ref[...], 0.0).astype(BF16)
    before = dot(node_hidden, nw2_ref[...]) + nb2_ref[...]
    node_out[...] = (fresh.astype(F32) + layer_norm(before, ng_ref[...], no_ref[...])).astype(BF16)
    for tile in range(tiles):
        spot = pl.ds(tile * TILE, TILE)
        pltpu.make_async_copy(new_buf.at[spot], edge_out.at[spot], out_sem.at[tile]).wait()


VM = pl.BlockSpec(memory_space=pltpu.VMEM)
ANY = pl.BlockSpec(memory_space=pl.ANY)


def exchange(count, old, mig_send, mig_recv, halo_send, cross_send):
    nodes = old.shape[0]
    far = halo_send.shape[1] + cross_send.shape[1]
    steps = 2 * R
    padded = jnp.pad(cross_send, ((0, 0), (0, 128 - cross_send.shape[1])), constant_values=nodes)
    return pl.pallas_call(
        functools.partial(exchange_kernel, count),
        out_shape=(jax.ShapeDtypeStruct((nodes, L), BF16), jax.ShapeDtypeStruct((far, L), BF16)),
        in_specs=[VM] * 5,
        out_specs=(VM, VM),
        scratch_shapes=[
            pltpu.VMEM((mig_send.shape[1], L), BF16),
            pltpu.VMEM((mig_send.shape[1], L), BF16),
            pltpu.VMEM((far, L), BF16),
            pltpu.VMEM((far, L), BF16),
            pltpu.SemaphoreType.DMA((steps,)),
            pltpu.SemaphoreType.DMA((steps,)),
            pltpu.SemaphoreType.DMA((steps + 1,)),
            pltpu.SemaphoreType.DMA((steps + 1,)),
        ],
        compiler_params=pltpu.CompilerParams(collective_id=0, has_side_effects=True, vmem_limit_bytes=16 << 20),
        name="exchange",
    )(old, mig_send, mig_recv.reshape(-1, 128), halo_send, padded)


def layer(fresh, halo, edge_latent, senders, receivers, edge_live, weights):
    nodes, edges = fresh.shape[0], edge_latent.shape[0]
    vectors = [w if w.ndim == 2 else w.reshape(1, -1) for w in weights]
    lines = [v.reshape(-1, 128) for v in (senders, receivers, edge_live)]
    return pl.pallas_call(
        layer_kernel,
        out_shape=(jax.ShapeDtypeStruct((nodes, L), BF16), jax.ShapeDtypeStruct((edges, L), BF16)),
        in_specs=[VM] * (5 + len(vectors)) + [ANY],
        out_specs=(VM, ANY),
        scratch_shapes=[
            pltpu.VMEM((edges, L), BF16),
            pltpu.VMEM((edges, L), BF16),
            pltpu.VMEM((HALF + 256, 2 * L), BF16),
            pltpu.VMEM((HALF, 2 * L), BF16),
            pltpu.VMEM((edges // 128, 128), I32),
            pltpu.VMEM((2, TILE, L), F32),
            pltpu.VMEM((HALF, 2 * L), F32),
            pltpu.SemaphoreType.DMA((edges // TILE,)),
            pltpu.SemaphoreType.DMA((edges // TILE,)),
        ],
        compiler_params=pltpu.CompilerParams(vmem_limit_bytes=40 << 20),
        name="layer",
    )(fresh, halo, *lines, *vectors, edge_latent)


def solution(mesh):
    count = mesh.shape["dom"]

    def body(node_latent, edge_latent, mig_send, mig_recv, halo_send, cross_send, senders, receivers, edge_live,
             *weights):
        fresh, halo = exchange(count, node_latent, mig_send, mig_recv, halo_send, cross_send)
        return layer(fresh, halo, edge_latent, senders, receivers, edge_live, weights)

    rows, line = P(("grp", "dom"), None), P(("grp", "dom"))
    return jax.shard_map(
        body,
        mesh=mesh,
        in_specs=(rows, rows, rows, line, rows, rows, line, line, line) + (P(),) * 12,
        out_specs=(rows, rows),
        check_vma=False,
    )
```

```python
import functools

import jax
import jax.numpy as jnp
from jax import lax
from jax.experimental import pallas as pl
from jax.experimental.pallas import tpu as pltpu
from jax.sharding import PartitionSpec as P

R = 2
EPSILON = 1e-05
L = 128
HALF = 512
WORD_TILE = 512
GATHER_TILE = 1024
TILE = 1024
MESH = pl.DeviceIdType.MESH
F32, BF16, I32, I16 = jnp.float32, jnp.bfloat16, jnp.int32, jnp.int16
UPPER_S, UPPER_R, LIVE = 30, 29, 28


def offset_list():
    return [number - R if number < R else number - R + 1 for number in range(2 * R)]


def dot(a, b):
    return jnp.dot(a, b, preferred_element_type=F32)


def down(row):
    return jnp.broadcast_to(row, (128, 128)).T


def lanes_from(first):
    return (lax.broadcasted_iota(I32, (16, 128), 1) + first).astype(I16)


def one_hot(column, first, width):
    pieces = []
    for start in range(0, width, 128):
        lanes = jnp.concatenate([lanes_from(first + start)] * (column.shape[0] // 16), axis=0)
        pieces.append(jnp.where(column == lanes, jnp.bfloat16(1), jnp.bfloat16(0)))
    return jnp.concatenate(pieces, axis=1) if len(pieces) > 1 else pieces[0]


def layer_norm(values, gain, bias):
    center = values - jnp.mean(values, axis=-1, keepdims=True)
    spread = jnp.mean(center * center, axis=-1, keepdims=True)
    return center * lax.rsqrt(spread + EPSILON) * gain + bias


def spot_of(step, size):
    return pl.ds(pl.multiple_of(step * size, size), size)


def exchange_kernel(count, old_hbm, ms_hbm, mr_hbm, hs_hbm, xs_hbm, snd_hbm, rcv_hbm, live_hbm, edge_hbm, *rest):
    weights_hbm, rest = rest[:12], rest[12:]
    fresh_ref, far_ref, pre_ref, words_ref, send_ref, rows_ref, edge_ref = rest[:7]
    weights = rest[7:19]
    (old_ref, ms_ref, mr_ref, hs_ref, xs_ref, snd_ref, rcv_ref, live_ref, recv_ref, send_tab, recv_tab,
     leave_buf, arrive_buf, out_buf, in_buf, in_sem, w_sem, lsend, lrecv, hsend, hrecv) = rest[19:]
    shifts = offset_list()
    steps = len(shifts)
    loads = [pltpu.make_async_copy(src, dst, in_sem.at[i]) for i, (src, dst) in enumerate([
        (ms_hbm, ms_ref), (old_hbm, old_ref), (mr_hbm, mr_ref), (hs_hbm, hs_ref), (xs_hbm, xs_ref),
        (snd_hbm, snd_ref), (rcv_hbm, rcv_ref), (live_hbm, live_ref), (edge_hbm, edge_ref)])]
    loads += [pltpu.make_async_copy(src, dst, w_sem.at[i]) for i, (src, dst) in enumerate(zip(weights_hbm, weights))]

    arrive_buf[...] = jnp.zeros_like(arrive_buf)
    in_buf[...] = jnp.zeros_like(in_buf)
    if count:
        me = lax.axis_index("dom")
        other = 1 - lax.axis_index("grp")
        there = [(me + shift >= 0) & (me + shift < count) for shift in shifts]
        peers = [jnp.clip(me + shift, 0, count - 1) for shift in shifts]
        barrier = pltpu.get_barrier_semaphore()
        for peer, real in zip(peers, there):
            @pl.when(real)
            def _():
                pl.semaphore_signal(barrier, inc=1, device_id={"dom": peer}, device_id_type=MESH)
        pl.semaphore_signal(barrier, inc=1, device_id={"grp": other}, device_id_type=MESH)

    for load in loads:
        load.start()
    nodes = old_ref.shape[0]
    moves = ms_ref.shape[1] // steps
    halos = hs_ref.shape[1] // steps
    across = xs_ref.shape[1]
    loads[0].wait()
    want = jnp.concatenate([down(ms_ref[:, i:i + 128]) for i in range(0, ms_ref.shape[1], 128)], axis=0).astype(I16)
    hot = one_hot(want, 0, nodes)
    loads[1].wait()
    old = old_ref[...]
    leave_buf[...] = dot(hot, old).astype(BF16)

    def sends(src, dst, size, send_sem, recv_sem):
        made = []
        for place in range(steps):
            rows = pl.ds(place * size, size)
            made.append(pltpu.make_async_remote_copy(
                src_ref=src.at[rows], dst_ref=dst.at[rows], send_sem=send_sem.at[place], recv_sem=recv_sem.at[place],
                device_id={"dom": peers[place]}, device_id_type=MESH))
        return made

    if count:
        from_there = [there[steps - 1 - place] for place in range(steps)]
        pl.semaphore_wait(barrier, sum(real.astype(I32) for real in there) + 1)
        first = sends(leave_buf, arrive_buf, moves, lsend, lrecv)
        for copy, real in zip(first, there):
            pl.when(real)(copy.start)

    for load in loads[2:8]:
        load.wait()
    take = jnp.concatenate([down(mr_ref[i:i + 1, :]) for i in range(mr_ref.shape[0])], axis=0).astype(I16)
    stay_hot = one_hot(take, 0, nodes)
    new_hot = one_hot(take, nodes, arrive_buf.shape[0])
    hwant = jnp.concatenate([down(hs_ref[...]),
                             down(jnp.concatenate([xs_ref[...]] * (128 // across), axis=1))[:across]],
                            axis=0).astype(I16)
    halo_hot = one_hot(hwant, 0, nodes)
    via_new = dot(halo_hot, new_hot).astype(BF16)
    stay = dot(stay_hot, old)
    halo_stay = dot(halo_hot, stay.astype(BF16))

    s, r, live = snd_ref[...], rcv_ref[...], live_ref[...]
    far_s = s >= 2 * HALF
    s_row = jnp.where(far_s, s - HALF, s & (HALF - 1))
    s_up = jnp.where(far_s, 0, s >> 9)
    r_row = r & (HALF - 1)
    rows_ref[...] = r_row
    snd_ref[...] = (s_row << 16) | r_row | (s_up << UPPER_S) | ((r >> 9) << UPPER_R) | (live << LIVE)
    for load in loads[8:]:
        load.wait()
    w1e, w1s, w1r = weights[0][0:L], weights[0][L:2 * L], weights[0][2 * L:3 * L]
    edges = edge_ref.shape[0]
    subs = WORD_TILE // 128

    @pl.loop(0, edges // WORD_TILE)
    def _(step):
        spot = spot_of(step, WORD_TILE)
        word = jnp.concatenate([down(snd_ref[pl.ds(step * subs + i, 1), :]) for i in range(subs)], axis=0)
        words_ref[spot] = word
        send_ref[spot] = ((word >> 16) & 1023).astype(I16)
        recv_ref[spot] = (word & 511).astype(I16)
        pre_ref[spot] = dot(edge_ref[spot], w1e) + weights[1][...]

    if count:
        for copy, real in zip(first, from_there):
            pl.when(real)(copy.wait_recv)
    else:
        arrive_buf[...] = leave_buf[...]
    new = arrive_buf[...]
    out_buf[...] = (halo_stay + dot(via_new, new)).astype(BF16)
    if count:
        second = sends(out_buf, in_buf, halos, hsend, hrecv)
        rows = pl.ds(steps * halos, across)
        swap = pltpu.make_async_remote_copy(
            src_ref=out_buf.at[rows], dst_ref=in_buf.at[rows],
            send_sem=hsend.at[steps], recv_sem=hrecv.at[steps],
            device_id={"grp": other}, device_id_type=MESH)
        for copy, real in zip(second, there):
            pl.when(real)(copy.start)
        swap.start()

    fresh = (stay + dot(new_hot, new)).astype(BF16)
    fresh_ref[...] = fresh
    part = dot(fresh, w1s).astype(BF16)
    send_tab[:, 0:L] = part[:HALF]
    send_tab[:, L:2 * L] = part[HALF:]
    part = dot(fresh, w1r).astype(BF16)
    recv_tab[:, 0:L] = part[:HALF]
    recv_tab[:, L:2 * L] = part[HALF:]

    @pl.loop(0, edges // GATHER_TILE)
    def _(step):
        spot = spot_of(step, GATHER_TILE)
        got_s = dot(one_hot(send_ref[spot], 0, HALF), send_tab[...])
        got_r = dot(one_hot(recv_ref[spot], 0, HALF), recv_tab[...])
        word = words_ref[spot]
        pre_ref[spot] = (pre_ref[spot] + jnp.where((word & (1 << UPPER_S)) != 0, got_s[:, L:], got_s[:, :L])
                         + jnp.where((word & (1 << UPPER_R)) != 0, got_r[:, L:], got_r[:, :L]))

    if count:
        for copy, real in zip(first, there):
            pl.when(real)(copy.wait_send)
        for copy, real in zip(second, there):
            pl.when(real)(copy.wait_send)
        for copy, real in zip(second, from_there):
            pl.when(real)(copy.wait_recv)
        swap.wait()
    else:
        in_buf[...] = out_buf[...]
    far = dot(in_buf[...], w1s).astype(BF16)
    far_ref[...] = jnp.concatenate([far, jnp.zeros((far_ref.shape[0] - far.shape[0], L), BF16)], axis=0)


def layer_kernel(fresh_ref, far_ref, pre_ref, words_ref, send_ref, rows_ref, edge_ref,
                 ew1_ref, eb1_ref, ew2_ref, eb2_ref, eg_ref, eo_ref,
                 nw1_ref, nb1_ref, nw2_ref, nb2_ref, ng_ref, no_ref,
                 node_out, edge_out, new_buf, side_0, side_1, sums, out_sem):
    edges = edge_ref.shape[0]
    tiles = edges // TILE
    subs = TILE // 128
    w2 = ew2_ref[...]
    nil = jnp.zeros((L, L), BF16)
    w2_pair = jnp.concatenate([jnp.concatenate([w2, nil], axis=1), jnp.concatenate([nil, w2], axis=1)], axis=0)
    sums[...] = jnp.zeros_like(sums)

    def messages(tile, side):
        spot = spot_of(tile, TILE)
        pre = pre_ref[spot] + dot(one_hot(send_ref[spot], HALF, 256), far_ref[...])
        hidden = jnp.maximum(pre, 0.0).astype(BF16)
        pair = jnp.concatenate([hidden[:TILE // 2], hidden[TILE // 2:]], axis=1)
        before = dot(pair, w2_pair)
        before = jnp.concatenate([before[:, :L], before[:, L:]], axis=0) + eb2_ref[...]
        message = layer_norm(before, eg_ref[...], eo_ref[...])
        word = words_ref[spot]
        kept = jnp.where((word & (1 << LIVE)) != 0, message, 0.0).astype(BF16)
        new_buf[spot] = (edge_ref[spot].astype(F32) + kept.astype(F32)).astype(BF16)
        upper = ((word >> 16) & (1 << (UPPER_R - 16))).astype(I16) != jnp.int16(0)
        zero = jnp.zeros_like(kept)
        side[:, 0:L] = jnp.where(upper, zero, kept)
        side[:, L:2 * L] = jnp.where(upper, kept, zero)

    def save(tile):
        spot = spot_of(tile, TILE)
        return pltpu.make_async_copy(new_buf.at[spot], edge_out.at[spot], out_sem.at[tile])

    def gather_in(tile, side):
        below = lax.broadcasted_iota(I32, (HALF, 128), 0).astype(I16)
        flat = []
        for i in range(subs):
            row = jnp.broadcast_to(rows_ref[pl.ds(tile * subs + i, 1), :], (16, 128)).astype(I16)
            row = jnp.concatenate([row] * (HALF // 16), axis=0)
            flat.append(jnp.where(row == below, jnp.bfloat16(1), jnp.bfloat16(0)))
        sums[...] += dot(jnp.concatenate(flat, axis=1), side[...])

    messages(0, side_0)

    @pl.loop(0, tiles // 2 - 1)
    def _(step):
        tile = 2 * step
        save(tile).start()
        gather_in(tile, side_0)
        messages(tile + 1, side_1)
        save(tile + 1).start()
        gather_in(tile + 1, side_1)
        messages(tile + 2, side_0)

    save(tiles - 2).start()
    gather_in(tiles - 2, side_0)
    messages(tiles - 1, side_1)
    save(tiles - 1).start()
    gather_in(tiles - 1, side_1)

    fresh = fresh_ref[...]
    inbound = jnp.concatenate([sums[:, :L], sums[:, L:]], axis=0).astype(BF16)
    node_hidden = jnp.maximum(dot(jnp.concatenate([fresh, inbound], axis=1), nw1_ref[...]) + nb1_ref[...], 0.0).astype(BF16)
    before = dot(node_hidden, nw2_ref[...]) + nb2_ref[...]
    node_out[...] = (fresh.astype(F32) + layer_norm(before, ng_ref[...], no_ref[...])).astype(BF16)
    for tile in range(tiles):
        save(tile).wait()


VM = pl.BlockSpec(memory_space=pltpu.VMEM)
ANY = pl.BlockSpec(memory_space=pl.ANY)
HBM = pl.BlockSpec(memory_space=pltpu.HBM)


def in_hbm(x):
    return pltpu.with_memory_space_constraint(x, pltpu.HBM)


def exchange(count, old, mig_send, mig_recv, halo_send, cross_send, lines, edge_latent, vectors):
    nodes, edges = old.shape[0], edge_latent.shape[0]
    far = halo_send.shape[1] + cross_send.shape[1]
    steps = 2 * R
    kept = [((nodes, L), BF16), ((256, L), BF16), ((edges, L), F32), ((edges, L), I32), ((edges, L), I16),
            (lines[0].shape, I32), ((edges, L), BF16)] + [(v.shape, v.dtype) for v in vectors]
    operands = [old, mig_send, mig_recv.reshape(-1, 128), halo_send, cross_send, *lines, edge_latent, *vectors]
    params = dict(collective_id=0) if count else {}
    return pl.pallas_call(
        functools.partial(exchange_kernel, count),
        out_shape=tuple(pltpu.VMEM(shape, dtype) for shape, dtype in kept),
        in_specs=[HBM] * len(operands),
        out_specs=(VM,) * len(kept),
        scratch_shapes=[
            pltpu.VMEM(old.shape, BF16), pltpu.VMEM(mig_send.shape, I32), pltpu.VMEM((nodes // 128, 128), I32),
            pltpu.VMEM(halo_send.shape, I32), pltpu.VMEM(cross_send.shape, I32),
            pltpu.VMEM(lines[0].shape, I32), pltpu.VMEM(lines[0].shape, I32), pltpu.VMEM(lines[0].shape, I32),
            pltpu.VMEM((edges, L), I16),
            pltpu.VMEM((HALF, 2 * L), BF16), pltpu.VMEM((HALF, 2 * L), BF16),
            pltpu.VMEM((mig_send.shape[1], L), BF16), pltpu.VMEM((mig_send.shape[1], L), BF16),
            pltpu.VMEM((far, L), BF16), pltpu.VMEM((far, L), BF16),
            pltpu.SemaphoreType.DMA((9,)), pltpu.SemaphoreType.DMA((len(vectors),)),
            pltpu.SemaphoreType.DMA((steps,)), pltpu.SemaphoreType.DMA((steps,)),
            pltpu.SemaphoreType.DMA((steps + 1,)), pltpu.SemaphoreType.DMA((steps + 1,)),
        ],
        compiler_params=pltpu.CompilerParams(has_side_effects=True, vmem_limit_bytes=24 << 20, **params),
        name="exchange",
    )(*[in_hbm(x) for x in operands])


def layer(parts):
    nodes, edges = parts[0].shape[0], parts[2].shape[0]
    return pl.pallas_call(
        layer_kernel,
        out_shape=(jax.ShapeDtypeStruct((nodes, L), BF16), pltpu.HBM((edges, L), BF16)),
        in_specs=[VM] * len(parts),
        out_specs=(VM, HBM),
        scratch_shapes=[
            pltpu.VMEM((edges, L), BF16),
            pltpu.VMEM((TILE, 2 * L), BF16),
            pltpu.VMEM((TILE, 2 * L), BF16),
            pltpu.VMEM((HALF, 2 * L), F32),
            pltpu.SemaphoreType.DMA((edges // TILE,)),
        ],
        compiler_params=pltpu.CompilerParams(vmem_limit_bytes=24 << 20),
        name="layer",
    )(*parts)


def step(count, node_latent, edge_latent, mig_send, mig_recv, halo_send, cross_send, senders, receivers, edge_live,
         *weights):
    vectors = [w if w.ndim == 2 else w.reshape(1, -1) for w in weights]
    lines = [v.reshape(-1, 128) for v in (senders, receivers, edge_live)]
    return layer(exchange(count, node_latent, mig_send, mig_recv, halo_send, cross_send, lines, edge_latent, vectors))


def solution(mesh):
    rows, line = P(("grp", "dom"), None), P(("grp", "dom"))
    return jax.shard_map(
        functools.partial(step, mesh.shape["dom"]),
        mesh=mesh,
        in_specs=(rows, rows, rows, line, rows, rows, line, line, line) + (P(),) * 12,
        out_specs=(rows, rows),
        check_vma=False,
    )
```

```python
import functools

import jax
import jax.numpy as jnp
from jax import lax
from jax.experimental import pallas as pl
from jax.experimental.pallas import tpu as pltpu
from jax.sharding import PartitionSpec as P

R = 2
EPSILON = 1e-05
L = 128
HALF = 512
WORD_TILE = 1536
GATHER_TILE = 3072
TILE = 3072
MESH = pl.DeviceIdType.MESH
F32, BF16, I32, I16 = jnp.float32, jnp.bfloat16, jnp.int32, jnp.int16
UPPER_S, UPPER_R, LIVE = 30, 29, 28
EARLY = 6


def offset_list():
    return [number - R if number < R else number - R + 1 for number in range(2 * R)]


def dot(a, b):
    return jnp.dot(a, b, preferred_element_type=F32)


def down(row):
    return jnp.broadcast_to(row, (128, 128)).T


def lanes_from(first):
    return (lax.broadcasted_iota(I32, (16, 128), 1) + first).astype(I16)


def one_hot(column, first, width):
    pieces = []
    for start in range(0, width, 128):
        lanes = jnp.concatenate([lanes_from(first + start)] * (column.shape[0] // 16), axis=0)
        pieces.append(jnp.where(column == lanes, jnp.bfloat16(1), jnp.bfloat16(0)))
    return jnp.concatenate(pieces, axis=1) if len(pieces) > 1 else pieces[0]


def layer_norm(values, gain, bias):
    center = values - jnp.mean(values, axis=-1, keepdims=True)
    spread = jnp.mean(center * center, axis=-1, keepdims=True)
    return center * lax.rsqrt(spread + EPSILON) * gain + bias


def spot_of(step, size):
    return pl.ds(pl.multiple_of(step * size, size), size)


def exchange_kernel(count, old_hbm, ms_hbm, mr_hbm, hs_hbm, xs_hbm, snd_hbm, rcv_hbm, live_hbm, edge_hbm, *rest):
    weights_hbm, rest = rest[:12], rest[12:]
    fresh_ref, far_ref, pre_ref, send_ref, code_ref, rows_ref, edge_ref = rest[:7]
    weights = rest[7:19]
    (old_ref, ms_ref, mr_ref, hs_ref, xs_ref, snd_ref, rcv_ref, live_ref, words_ref, recv_ref, send_tab, recv_tab,
     leave_buf, arrive_buf, out_buf, in_buf, stay_buf, new_buf, via_buf, halo_buf, in_sem, w_sem, lsend, lrecv, hsend, hrecv) = rest[19:]
    shifts = offset_list()
    steps = len(shifts)
    loads = [pltpu.make_async_copy(src, dst, in_sem.at[i]) for i, (src, dst) in enumerate([
        (ms_hbm, ms_ref), (old_hbm, old_ref), (mr_hbm, mr_ref), (hs_hbm, hs_ref), (xs_hbm, xs_ref),
        (snd_hbm, snd_ref), (rcv_hbm, rcv_ref), (live_hbm, live_ref), (edge_hbm, edge_ref)])]
    loads += [pltpu.make_async_copy(src, dst, w_sem.at[i]) for i, (src, dst) in enumerate(zip(weights_hbm, weights))]

    arrive_buf[...] = jnp.zeros_like(arrive_buf)
    in_buf[...] = jnp.zeros_like(in_buf)
    if count:
        me = lax.axis_index("dom")
        other = 1 - lax.axis_index("grp")
        there = [(me + shift >= 0) & (me + shift < count) for shift in shifts]
        peers = [jnp.clip(me + shift, 0, count - 1) for shift in shifts]
        barrier = pltpu.get_barrier_semaphore()
        for peer, real in zip(peers, there):
            @pl.when(real)
            def _():
                pl.semaphore_signal(barrier, inc=1, device_id={"dom": peer}, device_id_type=MESH)
        pl.semaphore_signal(barrier, inc=1, device_id={"grp": other}, device_id_type=MESH)

    for load in loads:
        load.start()
    nodes = old_ref.shape[0]
    moves = ms_ref.shape[1] // steps
    halos = hs_ref.shape[1] // steps
    across = xs_ref.shape[1]
    loads[0].wait()
    want = jnp.concatenate([down(ms_ref[:, i:i + 128]) for i in range(0, ms_ref.shape[1], 128)], axis=0).astype(I16)
    hot = one_hot(want, 0, nodes)
    loads[1].wait()
    old = old_ref[...]
    leave_buf[...] = dot(hot, old).astype(BF16)

    def sends(src, dst, size, send_sem, recv_sem):
        made = []
        for place in range(steps):
            rows = pl.ds(place * size, size)
            made.append(pltpu.make_async_remote_copy(
                src_ref=src.at[rows], dst_ref=dst.at[rows], send_sem=send_sem.at[place], recv_sem=recv_sem.at[place],
                device_id={"dom": peers[place]}, device_id_type=MESH))
        return made

    w1e, w1s, w1r = (weights[0].at[pl.ds(i * L, L)] for i in range(3))
    edges = edge_ref.shape[0]
    subs = WORD_TILE // 128

    def prepare():
        for load in loads[2:8]:
            load.wait()
        take = jnp.concatenate([down(mr_ref[i:i + 1, :]) for i in range(mr_ref.shape[0])], axis=0).astype(I16)
        new_hot = one_hot(take, nodes, arrive_buf.shape[0])
        hwant = jnp.concatenate([down(hs_ref[...]),
                                 down(jnp.concatenate([xs_ref[...]] * (128 // across), axis=1))[:across]],
                                axis=0).astype(I16)
        halo_hot = one_hot(hwant, 0, nodes)
        stay = dot(one_hot(take, 0, nodes), old_ref[...])
        new_buf[...] = new_hot
        via_buf[...] = dot(halo_hot, new_hot).astype(BF16)
        stay_buf[...] = stay
        halo_buf[...] = dot(halo_hot, stay.astype(BF16))

        s, r, live = snd_ref[...], rcv_ref[...], live_ref[...]
        far_s = s >= 2 * HALF
        s_row = jnp.where(far_s, s - HALF, s & (HALF - 1))
        s_up = jnp.where(far_s, 0, s >> 9)
        r_row = r & (HALF - 1)
        rows_ref[...] = r_row
        snd_ref[...] = (s_row << 16) | r_row | (s_up << UPPER_S) | ((r >> 9) << UPPER_R) | (live << LIVE)
        for load in loads[8:11]:
            load.wait()

        @pl.loop(0, edges // WORD_TILE)
        def _(step):
            spot = spot_of(step, WORD_TILE)
            word = jnp.concatenate([down(snd_ref[pl.ds(step * subs + i, 1), :]) for i in range(subs)], axis=0)
            words_ref[spot] = word
            send_ref[spot] = ((word >> 16) & 1023).astype(I16)
            recv_ref[spot] = (word & 511).astype(I16)
            code_ref[spot] = (jnp.where((word & (1 << LIVE)) != 0, word & 511, -1 - HALF)
                              + ((word >> (UPPER_R - 9)) & HALF)).astype(I16)
            pre_ref[spot] = dot(edge_ref[spot], w1e[...]) + weights[1][...]

    if count:
        from_there = [there[steps - 1 - place] for place in range(steps)]
        early = lax.rem(me, 8) < EARLY
        pl.when(early)(prepare)
        pl.semaphore_wait(barrier, sum(real.astype(I32) for real in there) + 1)
        first = sends(leave_buf, arrive_buf, moves, lsend, lrecv)
        for copy, real in zip(first, there):
            pl.when(real)(copy.start)
        pl.when(jnp.logical_not(early))(prepare)
    else:
        prepare()
    for load in loads[11:]:
        load.wait()

    if count:
        for copy, real in zip(first, from_there):
            pl.when(real)(copy.wait_recv)
    else:
        arrive_buf[...] = leave_buf[...]
    new = arrive_buf[...]
    out_buf[...] = (halo_buf[...] + dot(via_buf[...], new)).astype(BF16)
    if count:
        second = sends(out_buf, in_buf, halos, hsend, hrecv)
        rows = pl.ds(steps * halos, across)
        swap = pltpu.make_async_remote_copy(
            src_ref=out_buf.at[rows], dst_ref=in_buf.at[rows],
            send_sem=hsend.at[steps], recv_sem=hrecv.at[steps],
            device_id={"grp": other}, device_id_type=MESH)
        for copy, real in zip(second, there):
            pl.when(real)(copy.start)
        swap.start()

    fresh = (stay_buf[...] + dot(new_buf[...], new)).astype(BF16)
    fresh_ref[...] = fresh
    part = dot(fresh, w1s[...]).astype(BF16)
    send_tab[:, 0:L] = part[:HALF]
    send_tab[:, L:2 * L] = part[HALF:]
    part = dot(fresh, w1r[...]).astype(BF16)
    recv_tab[:, 0:L] = part[:HALF]
    recv_tab[:, L:2 * L] = part[HALF:]

    @pl.loop(0, edges // GATHER_TILE)
    def _(step):
        spot = spot_of(step, GATHER_TILE)
        got_s = dot(one_hot(send_ref[spot], 0, HALF), send_tab[...])
        got_r = dot(one_hot(recv_ref[spot], 0, HALF), recv_tab[...])
        word = words_ref[spot]
        pre_ref[spot] = (pre_ref[spot] + jnp.where((word & (1 << UPPER_S)) != 0, got_s[:, L:], got_s[:, :L])
                         + jnp.where((word & (1 << UPPER_R)) != 0, got_r[:, L:], got_r[:, :L]))

    if count:
        for copy, real in zip(first, there):
            pl.when(real)(copy.wait_send)
        for copy, real in zip(second, there):
            pl.when(real)(copy.wait_send)
        for copy, real in zip(second, from_there):
            pl.when(real)(copy.wait_recv)
        swap.wait()
    else:
        in_buf[...] = out_buf[...]
    far = dot(in_buf[...], w1s[...]).astype(BF16)
    far_ref[...] = jnp.concatenate([far, jnp.zeros((far_ref.shape[0] - far.shape[0], L), BF16)], axis=0)


def layer_kernel(fresh_ref, far_ref, pre_ref, send_ref, code_ref, rows_ref, edge_ref,
                 ew1_ref, eb1_ref, ew2_ref, eb2_ref, eg_ref, eo_ref,
                 nw1_ref, nb1_ref, nw2_ref, nb2_ref, ng_ref, no_ref,
                 node_out, edge_out, new_buf, side_0, side_1, sums, out_sem):
    edges = edge_ref.shape[0]
    tiles = edges // TILE
    subs = TILE // 128
    half = TILE // 2
    w2 = ew2_ref[...].astype(F32)
    w2 = (w2 - jnp.mean(w2, axis=-1, keepdims=True)).astype(BF16)
    b2 = eb2_ref[...] - jnp.mean(eb2_ref[...], axis=-1, keepdims=True)
    gain = eg_ref[...] * (L ** 0.5)
    nil = jnp.zeros((L, L), BF16)
    w2_pair = jnp.concatenate([jnp.concatenate([w2, nil], axis=1), jnp.concatenate([nil, w2], axis=1)], axis=0)
    sums[...] = jnp.zeros_like(sums)

    def messages(tile, side):
        spot = spot_of(tile, TILE)
        hot = one_hot(send_ref[spot], HALF, 256)
        pair = []
        for i in range(2):
            part = pre_ref[pl.ds(pl.multiple_of(tile * TILE + i * half, half), half)]
            part = part + dot(hot[i * half:(i + 1) * half], far_ref[...])
            pair.append(jnp.maximum(part.astype(BF16), jnp.bfloat16(0)))
        pair = jnp.concatenate(pair, axis=1)
        center = jnp.concatenate([dot(pair[:half // 2], w2_pair), dot(pair[half // 2:], w2_pair)], axis=0)
        center = jnp.concatenate([center[:, :L], center[:, L:]], axis=0) + b2
        total = jnp.sum(center * center, axis=-1, keepdims=True)
        message = (center * lax.rsqrt(total + EPSILON * L) * gain + eo_ref[...]).astype(BF16)
        code = code_ref[spot]
        zero = jnp.zeros_like(message)
        kept = jnp.where(code >= jnp.int16(0), message, zero)
        new_buf[spot] = edge_ref[spot] + kept
        lower = code < jnp.int16(HALF)
        side[:, 0:L] = jnp.where(lower, kept, zero)
        side[:, L:2 * L] = jnp.where(lower, zero, kept)

    def save(tile):
        spot = spot_of(tile, TILE)
        return pltpu.make_async_copy(new_buf.at[spot], edge_out.at[spot], out_sem.at[tile])

    def gather_in(tile, side):
        below = lax.broadcasted_iota(I32, (HALF, 128), 0).astype(I16)
        flat = []
        for i in range(subs):
            row = jnp.broadcast_to(rows_ref[pl.ds(tile * subs + i, 1), :], (16, 128)).astype(I16)
            row = jnp.concatenate([row] * (HALF // 16), axis=0)
            flat.append(jnp.where(row == below, jnp.bfloat16(1), jnp.bfloat16(0)))
        flat = jnp.concatenate(flat, axis=1)
        for i in range(2):
            rows = slice(i * (HALF // 2), (i + 1) * (HALF // 2))
            sums[rows] += dot(flat[rows], side[...])

    messages(0, side_0)

    @pl.loop(0, tiles // 2 - 1)
    def _(step):
        tile = 2 * step
        save(tile).start()
        gather_in(tile, side_0)
        messages(tile + 1, side_1)
        save(tile + 1).start()
        gather_in(tile + 1, side_1)
        messages(tile + 2, side_0)

    save(tiles - 2).start()
    gather_in(tiles - 2, side_0)
    messages(tiles - 1, side_1)
    save(tiles - 1).start()
    gather_in(tiles - 1, side_1)

    fresh = fresh_ref[...]
    inbound = jnp.concatenate([sums[:, :L], sums[:, L:]], axis=0).astype(BF16)
    node_in = jnp.concatenate([fresh, inbound], axis=1)
    half = fresh.shape[0] // 2
    for i in range(2):
        rows = slice(i * half, (i + 1) * half)
        hidden = jnp.maximum(dot(node_in[rows], nw1_ref[...]) + nb1_ref[...], 0.0).astype(BF16)
        before = dot(hidden, nw2_ref[...]) + nb2_ref[...]
        node_out[rows] = (fresh[rows].astype(F32) + layer_norm(before, ng_ref[...], no_ref[...])).astype(BF16)
    for tile in range(tiles):
        save(tile).wait()


VM = pl.BlockSpec(memory_space=pltpu.VMEM)
ANY = pl.BlockSpec(memory_space=pl.ANY)
HBM = pl.BlockSpec(memory_space=pltpu.HBM)


def in_hbm(x):
    return pltpu.with_memory_space_constraint(x, pltpu.HBM)


def exchange(count, old, mig_send, mig_recv, halo_send, cross_send, lines, edge_latent, vectors):
    nodes, edges = old.shape[0], edge_latent.shape[0]
    far = halo_send.shape[1] + cross_send.shape[1]
    steps = 2 * R
    kept = [((nodes, L), BF16), ((256, L), BF16), ((edges, L), F32), ((edges, L), I16), ((edges, L), I16),
            (lines[0].shape, I32), ((edges, L), BF16)] + [(v.shape, v.dtype) for v in vectors]
    operands = [old, mig_send, mig_recv.reshape(-1, 128), halo_send, cross_send, *lines, edge_latent, *vectors]
    params = dict(collective_id=0) if count else {}
    return pl.pallas_call(
        functools.partial(exchange_kernel, count),
        out_shape=tuple(pltpu.VMEM(shape, dtype) for shape, dtype in kept),
        in_specs=[HBM] * len(operands),
        out_specs=(VM,) * len(kept),
        scratch_shapes=[
            pltpu.VMEM(old.shape, BF16), pltpu.VMEM(mig_send.shape, I32), pltpu.VMEM((nodes // 128, 128), I32),
            pltpu.VMEM(halo_send.shape, I32), pltpu.VMEM(cross_send.shape, I32),
            pltpu.VMEM(lines[0].shape, I32), pltpu.VMEM(lines[0].shape, I32), pltpu.VMEM(lines[0].shape, I32),
            pltpu.VMEM((edges, L), I32), pltpu.VMEM((edges, L), I16),
            pltpu.VMEM((HALF, 2 * L), BF16), pltpu.VMEM((HALF, 2 * L), BF16),
            pltpu.VMEM((mig_send.shape[1], L), BF16), pltpu.VMEM((mig_send.shape[1], L), BF16),
            pltpu.VMEM((far, L), BF16), pltpu.VMEM((far, L), BF16),
            pltpu.VMEM((nodes, L), F32), pltpu.VMEM((nodes, mig_send.shape[1]), BF16),
            pltpu.VMEM((far, mig_send.shape[1]), BF16), pltpu.VMEM((far, L), F32),
            pltpu.SemaphoreType.DMA((9,)), pltpu.SemaphoreType.DMA((len(vectors),)),
            pltpu.SemaphoreType.DMA((steps,)), pltpu.SemaphoreType.DMA((steps,)),
            pltpu.SemaphoreType.DMA((steps + 1,)), pltpu.SemaphoreType.DMA((steps + 1,)),
        ],
        compiler_params=pltpu.CompilerParams(has_side_effects=True, vmem_limit_bytes=24 << 20, **params),
        name="exchange",
    )(*[in_hbm(x) for x in operands])


def layer(parts):
    nodes, edges = parts[0].shape[0], parts[2].shape[0]
    return pl.pallas_call(
        layer_kernel,
        out_shape=(jax.ShapeDtypeStruct((nodes, L), BF16), pltpu.HBM((edges, L), BF16)),
        in_specs=[VM] * len(parts),
        out_specs=(VM, HBM),
        scratch_shapes=[
            pltpu.VMEM((edges, L), BF16),
            pltpu.VMEM((TILE, 2 * L), BF16),
            pltpu.VMEM((TILE, 2 * L), BF16),
            pltpu.VMEM((HALF, 2 * L), F32),
            pltpu.SemaphoreType.DMA((edges // TILE,)),
        ],
        compiler_params=pltpu.CompilerParams(vmem_limit_bytes=24 << 20),
        name="layer",
    )(*parts)


def step(count, node_latent, edge_latent, mig_send, mig_recv, halo_send, cross_send, senders, receivers, edge_live,
         *weights):
    vectors = [w if w.ndim == 2 else w.reshape(1, -1) for w in weights]
    lines = [v.reshape(-1, 128) for v in (senders, receivers, edge_live)]
    return layer(exchange(count, node_latent, mig_send, mig_recv, halo_send, cross_send, lines, edge_latent, vectors))


def solution(mesh):
    rows, line = P(("grp", "dom"), None), P(("grp", "dom"))
    return jax.shard_map(
        functools.partial(step, mesh.shape["dom"]),
        mesh=mesh,
        in_specs=(rows, rows, rows, line, rows, rows, line, line, line) + (P(),) * 12,
        out_specs=(rows, rows),
        check_vma=False,
    )
```

```python
import functools

import jax
import jax.numpy as jnp
from jax import lax
from jax.experimental import pallas as pl
from jax.experimental.pallas import tpu as pltpu
from jax.sharding import PartitionSpec as P

R = 2
EPSILON = 1e-05
L = 128
HALF = 512
WORD_TILE = 1536
GATHER_TILE = 3072
TILE = 3072
MESH = pl.DeviceIdType.MESH
F32, BF16, I32, I16 = jnp.float32, jnp.bfloat16, jnp.int32, jnp.int16
UPPER_S, UPPER_R, LIVE = 30, 29, 28
EARLY = 6


def offset_list():
    return [number - R if number < R else number - R + 1 for number in range(2 * R)]


def dot(a, b):
    return jnp.dot(a, b, preferred_element_type=F32)


def down(row):
    return jnp.broadcast_to(row, (128, 128)).T


def lanes_from(first):
    return (lax.broadcasted_iota(I32, (16, 128), 1) + first).astype(I16)


def one_hot(column, first, width):
    pieces = []
    for start in range(0, width, 128):
        lanes = jnp.concatenate([lanes_from(first + start)] * (column.shape[0] // 16), axis=0)
        pieces.append(jnp.where(column == lanes, jnp.bfloat16(1), jnp.bfloat16(0)))
    return jnp.concatenate(pieces, axis=1) if len(pieces) > 1 else pieces[0]


def layer_norm(values, gain, bias):
    center = values - jnp.mean(values, axis=-1, keepdims=True)
    spread = jnp.mean(center * center, axis=-1, keepdims=True)
    return center * lax.rsqrt(spread + EPSILON) * gain + bias


def spot_of(step, size):
    return pl.ds(pl.multiple_of(step * size, size), size)


def exchange_kernel(count, old_hbm, ms_hbm, mr_hbm, hs_hbm, xs_hbm, snd_hbm, rcv_hbm, live_hbm, edge_hbm, *rest):
    weights_hbm, rest = rest[:12], rest[12:]
    fresh_ref, far_ref, pre_ref, send_ref, code_ref, rows_ref, edge_ref = rest[:7]
    weights = rest[7:19]
    (old_ref, ms_ref, mr_ref, hs_ref, xs_ref, snd_ref, rcv_ref, live_ref, words_ref, recv_ref, send_tab, recv_tab,
     leave_buf, arrive_buf, out_buf, in_buf, stay_buf, new_buf, via_buf, halo_buf, beside_buf, pick_buf, pick_in,
     in_sem, w_sem, lsend, lrecv, hsend, hrecv, bsend, brecv, psend, precv) = rest[19:]
    shifts = offset_list()
    steps = len(shifts)
    loads = [pltpu.make_async_copy(src, dst, in_sem.at[i]) for i, (src, dst) in enumerate([
        (ms_hbm, ms_ref), (old_hbm, old_ref), (mr_hbm, mr_ref), (hs_hbm, hs_ref), (xs_hbm, xs_ref),
        (snd_hbm, snd_ref), (rcv_hbm, rcv_ref), (live_hbm, live_ref), (edge_hbm, edge_ref)])]
    loads += [pltpu.make_async_copy(src, dst, w_sem.at[i]) for i, (src, dst) in enumerate(zip(weights_hbm, weights))]

    arrive_buf[...] = jnp.zeros_like(arrive_buf)
    in_buf[...] = jnp.zeros_like(in_buf)
    beside_buf[...] = jnp.zeros_like(beside_buf)
    pick_in[...] = jnp.zeros_like(pick_in)
    if count:
        me = lax.axis_index("dom")
        other = 1 - lax.axis_index("grp")
        there = [(me + shift >= 0) & (me + shift < count) for shift in shifts]
        peers = [jnp.clip(me + shift, 0, count - 1) for shift in shifts]
        barrier = pltpu.get_barrier_semaphore()
        for peer, real in zip(peers, there):
            @pl.when(real)
            def _():
                pl.semaphore_signal(barrier, inc=1, device_id={"dom": peer}, device_id_type=MESH)
        pl.semaphore_signal(barrier, inc=1, device_id={"grp": other}, device_id_type=MESH)

    for load in loads:
        load.start()
    nodes = old_ref.shape[0]
    moves = ms_ref.shape[1] // steps
    halos = hs_ref.shape[1] // steps
    across = xs_ref.shape[1]
    loads[0].wait()
    want = jnp.concatenate([down(ms_ref[:, i:i + 128]) for i in range(0, ms_ref.shape[1], 128)], axis=0).astype(I16)
    hot = one_hot(want, 0, nodes)
    loads[1].wait()
    old = old_ref[...]
    leave_buf[...] = dot(hot, old).astype(BF16)

    def sends(src, dst, size, send_sem, recv_sem):
        made = []
        for place in range(steps):
            rows = pl.ds(place * size, size)
            made.append(pltpu.make_async_remote_copy(
                src_ref=src.at[rows], dst_ref=dst.at[rows], send_sem=send_sem.at[place], recv_sem=recv_sem.at[place],
                device_id={"dom": peers[place]}, device_id_type=MESH))
        return made

    w1e, w1s, w1r = (weights[0].at[pl.ds(i * L, L)] for i in range(3))
    edges = edge_ref.shape[0]
    subs = WORD_TILE // 128
    ahead_rows, behind_rows = pl.ds(0, 2 * moves), pl.ds(2 * moves, 2 * moves)

    def plan_rows():
        for load in loads[2:5]:
            load.wait()
        take = jnp.concatenate([down(mr_ref[i:i + 1, :]) for i in range(mr_ref.shape[0])], axis=0).astype(I16)
        new_hot = one_hot(take, nodes, arrive_buf.shape[0])
        hwant = jnp.concatenate([down(hs_ref[...]),
                                 down(jnp.concatenate([xs_ref[...]] * (128 // across), axis=1))[:across]],
                                axis=0).astype(I16)
        halo_hot = one_hot(hwant, 0, nodes)
        stay = dot(one_hot(take, 0, nodes), old_ref[...])
        new_buf[...] = new_hot
        via = dot(halo_hot, new_hot).astype(BF16)
        via_buf[...] = via
        pick_buf[0:2 * halos] = via[0:2 * halos, 2 * moves:]
        pick_buf[2 * halos:4 * halos] = via[2 * halos:4 * halos, :2 * moves]
        stay_buf[...] = stay
        halo_buf[...] = dot(halo_hot, stay.astype(BF16))

    def plan_edges():
        for load in loads[5:8]:
            load.wait()
        s, r, live = snd_ref[...], rcv_ref[...], live_ref[...]
        far_s = s >= 2 * HALF
        s_row = jnp.where(far_s, s - HALF, s & (HALF - 1))
        s_up = jnp.where(far_s, 0, s >> 9)
        r_row = r & (HALF - 1)
        rows_ref[...] = r_row
        snd_ref[...] = (s_row << 16) | r_row | (s_up << UPPER_S) | ((r >> 9) << UPPER_R) | (live << LIVE)
        for load in loads[8:11]:
            load.wait()

        @pl.loop(0, edges // WORD_TILE)
        def _(step):
            spot = spot_of(step, WORD_TILE)
            word = jnp.concatenate([down(snd_ref[pl.ds(step * subs + i, 1), :]) for i in range(subs)], axis=0)
            words_ref[spot] = word
            send_ref[spot] = ((word >> 16) & 1023).astype(I16)
            recv_ref[spot] = (word & 511).astype(I16)
            code_ref[spot] = (jnp.where((word & (1 << LIVE)) != 0, word & 511, -1 - HALF)
                              + ((word >> (UPPER_R - 9)) & HALF)).astype(I16)
            pre_ref[spot] = dot(edge_ref[spot], w1e[...]) + weights[1][...]

    def start(copies, conditions):
        for copy, real in zip(copies, conditions):
            pl.when(real)(copy.start)

    def arrived(copies, conditions):
        for copy, real in zip(copies, conditions):
            pl.when(real)(copy.wait_recv)

    if count:
        from_there = [there[steps - 1 - place] for place in range(steps)]
        before_us, after_us = there[R - 1], there[R]
        early = lax.rem(me, 8) < EARLY

        @pl.when(early)
        def _():
            plan_rows()
            plan_edges()

        pl.semaphore_wait(barrier, sum(real.astype(I32) for real in there) + 1)
        first = sends(leave_buf, arrive_buf, moves, lsend, lrecv)
        start(first, there)
        shared = []
        for place in range(steps):
            rows = pl.ds(place * moves, moves)
            shared.append(pltpu.make_async_remote_copy(
                src_ref=leave_buf.at[rows], dst_ref=beside_buf.at[rows],
                send_sem=bsend.at[place], recv_sem=brecv.at[place],
                device_id={"dom": peers[R - 1] if place % 2 == 0 else peers[R]}, device_id_type=MESH))
        shared_to = [before_us, after_us] * R
        shared_from = [after_us, before_us] * R
        start(shared, shared_to)

        @pl.when(jnp.logical_not(early))
        def _():
            plan_rows()

        picks = sends(pick_buf, pick_in, halos, psend, precv)
        start(picks, there)
        second = sends(out_buf, in_buf, halos, hsend, hrecv)
        rows = pl.ds(steps * halos, across)
        swap = pltpu.make_async_remote_copy(
            src_ref=out_buf.at[rows], dst_ref=in_buf.at[rows],
            send_sem=hsend.at[steps], recv_sem=hrecv.at[steps],
            device_id={"grp": other}, device_id_type=MESH)

        arrived(first[R:], from_there[R:])
        slots = pl.ds(2 * halos, 2 * halos)
        out_buf[slots] = (halo_buf[slots] + dot(via_buf[slots, 2 * moves:], arrive_buf[behind_rows])).astype(BF16)
        start(second[R:], there[R:])

        @pl.when(jnp.logical_not(early))
        def _():
            plan_edges()

        arrived(first[:R], from_there[:R])
        slots = pl.ds(0, 2 * halos)
        out_buf[slots] = (halo_buf[slots] + dot(via_buf[slots, :2 * moves], arrive_buf[ahead_rows])).astype(BF16)
        start(second[:R], there[:R])
        out_buf[rows] = (halo_buf[rows] + dot(via_buf[rows], arrive_buf[...])).astype(BF16)
        swap.start()
    else:
        plan_rows()
        plan_edges()
        arrive_buf[...] = leave_buf[...]
        out_buf[...] = (halo_buf[...] + dot(via_buf[...], arrive_buf[...])).astype(BF16)
    for load in loads[11:]:
        load.wait()
    new = arrive_buf[...]

    fresh = (stay_buf[...] + dot(new_buf[...], new)).astype(BF16)
    fresh_ref[...] = fresh
    part = dot(fresh, w1s[...]).astype(BF16)
    send_tab[:, 0:L] = part[:HALF]
    send_tab[:, L:2 * L] = part[HALF:]
    part = dot(fresh, w1r[...]).astype(BF16)
    recv_tab[:, 0:L] = part[:HALF]
    recv_tab[:, L:2 * L] = part[HALF:]

    @pl.loop(0, edges // GATHER_TILE)
    def _(step):
        spot = spot_of(step, GATHER_TILE)
        got_s = dot(one_hot(send_ref[spot], 0, HALF), send_tab[...])
        got_r = dot(one_hot(recv_ref[spot], 0, HALF), recv_tab[...])
        word = words_ref[spot]
        pre_ref[spot] = (pre_ref[spot] + jnp.where((word & (1 << UPPER_S)) != 0, got_s[:, L:], got_s[:, :L])
                         + jnp.where((word & (1 << UPPER_R)) != 0, got_r[:, L:], got_r[:, :L]))

    if count:
        for copies, conditions in ((first, there), (shared, shared_to), (picks, there), (second, there)):
            for copy, real in zip(copies, conditions):
                pl.when(real)(copy.wait_send)
        arrived(shared, shared_from)
        arrived(picks, from_there)
        arrived(second, from_there)
        swap.wait()

        def list_of(buf, place):
            return buf[place * moves:(place + 1) * moves]

        filled = []
        for place, (one, two) in enumerate((((beside_buf, 2), (leave_buf, 3)), ((leave_buf, 2), (beside_buf, 3)),
                                            ((beside_buf, 0), (leave_buf, 1)), ((leave_buf, 0), (beside_buf, 1)))):
            rows = pl.ds(place * halos, halos)
            table = jnp.concatenate([list_of(*one), list_of(*two)], axis=0)
            filled.append((in_buf[rows].astype(F32) + dot(pick_in[rows], table)).astype(BF16))
        halo = jnp.concatenate(filled + [in_buf[pl.ds(steps * halos, across)]], axis=0)
    else:
        halo = out_buf[...]
    far = dot(halo, w1s[...]).astype(BF16)
    far_ref[...] = jnp.concatenate([far, jnp.zeros((far_ref.shape[0] - far.shape[0], L), BF16)], axis=0)


def layer_kernel(fresh_ref, far_ref, pre_ref, send_ref, code_ref, rows_ref, edge_ref,
                 ew1_ref, eb1_ref, ew2_ref, eb2_ref, eg_ref, eo_ref,
                 nw1_ref, nb1_ref, nw2_ref, nb2_ref, ng_ref, no_ref,
                 node_out, edge_out, new_buf, side_0, side_1, sums, out_sem):
    edges = edge_ref.shape[0]
    tiles = edges // TILE
    subs = TILE // 128
    half = TILE // 2
    w2 = ew2_ref[...].astype(F32)
    w2 = (w2 - jnp.mean(w2, axis=-1, keepdims=True)).astype(BF16)
    b2 = eb2_ref[...] - jnp.mean(eb2_ref[...], axis=-1, keepdims=True)
    gain = eg_ref[...] * (L ** 0.5)
    nil = jnp.zeros((L, L), BF16)
    w2_pair = jnp.concatenate([jnp.concatenate([w2, nil], axis=1), jnp.concatenate([nil, w2], axis=1)], axis=0)
    sums[...] = jnp.zeros_like(sums)

    def messages(tile, side):
        spot = spot_of(tile, TILE)
        hot = one_hot(send_ref[spot], HALF, 256)
        pair = []
        for i in range(2):
            part = pre_ref[pl.ds(pl.multiple_of(tile * TILE + i * half, half), half)]
            part = part + dot(hot[i * half:(i + 1) * half], far_ref[...])
            pair.append(jnp.maximum(part.astype(BF16), jnp.bfloat16(0)))
        pair = jnp.concatenate(pair, axis=1)
        center = jnp.concatenate([dot(pair[:half // 2], w2_pair), dot(pair[half // 2:], w2_pair)], axis=0)
        center = jnp.concatenate([center[:, :L], center[:, L:]], axis=0) + b2
        total = jnp.sum(center * center, axis=-1, keepdims=True)
        message = (center * lax.rsqrt(total + EPSILON * L) * gain + eo_ref[...]).astype(BF16)
        code = code_ref[spot]
        zero = jnp.zeros_like(message)
        kept = jnp.where(code >= jnp.int16(0), message, zero)
        new_buf[spot] = edge_ref[spot] + kept
        lower = code < jnp.int16(HALF)
        side[:, 0:L] = jnp.where(lower, kept, zero)
        side[:, L:2 * L] = jnp.where(lower, zero, kept)

    def save(tile):
        spot = spot_of(tile, TILE)
        return pltpu.make_async_copy(new_buf.at[spot], edge_out.at[spot], out_sem.at[tile])

    def gather_in(tile, side):
        below = lax.broadcasted_iota(I32, (HALF, 128), 0).astype(I16)
        flat = []
        for i in range(subs):
            row = jnp.broadcast_to(rows_ref[pl.ds(tile * subs + i, 1), :], (16, 128)).astype(I16)
            row = jnp.concatenate([row] * (HALF // 16), axis=0)
            flat.append(jnp.where(row == below, jnp.bfloat16(1), jnp.bfloat16(0)))
        flat = jnp.concatenate(flat, axis=1)
        for i in range(2):
            rows = slice(i * (HALF // 2), (i + 1) * (HALF // 2))
            sums[rows] += dot(flat[rows], side[...])

    messages(0, side_0)

    @pl.loop(0, tiles // 2 - 1)
    def _(step):
        tile = 2 * step
        save(tile).start()
        gather_in(tile, side_0)
        messages(tile + 1, side_1)
        save(tile + 1).start()
        gather_in(tile + 1, side_1)
        messages(tile + 2, side_0)

    save(tiles - 2).start()
    gather_in(tiles - 2, side_0)
    messages(tiles - 1, side_1)
    save(tiles - 1).start()
    gather_in(tiles - 1, side_1)

    fresh = fresh_ref[...]
    inbound = jnp.concatenate([sums[:, :L], sums[:, L:]], axis=0).astype(BF16)
    node_in = jnp.concatenate([fresh, inbound], axis=1)
    half = fresh.shape[0] // 2
    for i in range(2):
        rows = slice(i * half, (i + 1) * half)
        hidden = jnp.maximum(dot(node_in[rows], nw1_ref[...]) + nb1_ref[...], 0.0).astype(BF16)
        before = dot(hidden, nw2_ref[...]) + nb2_ref[...]
        node_out[rows] = (fresh[rows].astype(F32) + layer_norm(before, ng_ref[...], no_ref[...])).astype(BF16)
    for tile in range(tiles):
        save(tile).wait()


VM = pl.BlockSpec(memory_space=pltpu.VMEM)
ANY = pl.BlockSpec(memory_space=pl.ANY)
HBM = pl.BlockSpec(memory_space=pltpu.HBM)


def in_hbm(x):
    return pltpu.with_memory_space_constraint(x, pltpu.HBM)


def exchange(count, old, mig_send, mig_recv, halo_send, cross_send, lines, edge_latent, vectors):
    nodes, edges = old.shape[0], edge_latent.shape[0]
    far = halo_send.shape[1] + cross_send.shape[1]
    steps = 2 * R
    kept = [((nodes, L), BF16), ((256, L), BF16), ((edges, L), F32), ((edges, L), I16), ((edges, L), I16),
            (lines[0].shape, I32), ((edges, L), BF16)] + [(v.shape, v.dtype) for v in vectors]
    operands = [old, mig_send, mig_recv.reshape(-1, 128), halo_send, cross_send, *lines, edge_latent, *vectors]
    params = dict(collective_id=0) if count else {}
    return pl.pallas_call(
        functools.partial(exchange_kernel, count),
        out_shape=tuple(pltpu.VMEM(shape, dtype) for shape, dtype in kept),
        in_specs=[HBM] * len(operands),
        out_specs=(VM,) * len(kept),
        scratch_shapes=[
            pltpu.VMEM(old.shape, BF16), pltpu.VMEM(mig_send.shape, I32), pltpu.VMEM((nodes // 128, 128), I32),
            pltpu.VMEM(halo_send.shape, I32), pltpu.VMEM(cross_send.shape, I32),
            pltpu.VMEM(lines[0].shape, I32), pltpu.VMEM(lines[0].shape, I32), pltpu.VMEM(lines[0].shape, I32),
            pltpu.VMEM((edges, L), I32), pltpu.VMEM((edges, L), I16),
            pltpu.VMEM((HALF, 2 * L), BF16), pltpu.VMEM((HALF, 2 * L), BF16),
            pltpu.VMEM((mig_send.shape[1], L), BF16), pltpu.VMEM((mig_send.shape[1], L), BF16),
            pltpu.VMEM((far, L), BF16), pltpu.VMEM((far, L), BF16),
            pltpu.VMEM((nodes, L), F32), pltpu.VMEM((nodes, mig_send.shape[1]), BF16),
            pltpu.VMEM((far, mig_send.shape[1]), BF16), pltpu.VMEM((far, L), F32),
            pltpu.VMEM((mig_send.shape[1], L), BF16), pltpu.VMEM((halo_send.shape[1], 128), BF16),
            pltpu.VMEM((halo_send.shape[1], 128), BF16),
            pltpu.SemaphoreType.DMA((9,)), pltpu.SemaphoreType.DMA((len(vectors),)),
            pltpu.SemaphoreType.DMA((steps,)), pltpu.SemaphoreType.DMA((steps,)),
            pltpu.SemaphoreType.DMA((steps + 1,)), pltpu.SemaphoreType.DMA((steps + 1,)),
            *[pltpu.SemaphoreType.DMA((steps,))] * 4,
        ],
        compiler_params=pltpu.CompilerParams(has_side_effects=True, vmem_limit_bytes=24 << 20, **params),
        name="exchange",
    )(*[in_hbm(x) for x in operands])


def layer(parts):
    nodes, edges = parts[0].shape[0], parts[2].shape[0]
    return pl.pallas_call(
        layer_kernel,
        out_shape=(jax.ShapeDtypeStruct((nodes, L), BF16), pltpu.HBM((edges, L), BF16)),
        in_specs=[VM] * len(parts),
        out_specs=(VM, HBM),
        scratch_shapes=[
            pltpu.VMEM((edges, L), BF16),
            pltpu.VMEM((TILE, 2 * L), BF16),
            pltpu.VMEM((TILE, 2 * L), BF16),
            pltpu.VMEM((HALF, 2 * L), F32),
            pltpu.SemaphoreType.DMA((edges // TILE,)),
        ],
        compiler_params=pltpu.CompilerParams(vmem_limit_bytes=24 << 20),
        name="layer",
    )(*parts)


def step(count, node_latent, edge_latent, mig_send, mig_recv, halo_send, cross_send, senders, receivers, edge_live,
         *weights):
    vectors = [w if w.ndim == 2 else w.reshape(1, -1) for w in weights]
    lines = [v.reshape(-1, 128) for v in (senders, receivers, edge_live)]
    return layer(exchange(count, node_latent, mig_send, mig_recv, halo_send, cross_send, lines, edge_latent, vectors))


def solution(mesh):
    rows, line = P(("grp", "dom"), None), P(("grp", "dom"))
    return jax.shard_map(
        functools.partial(step, mesh.shape["dom"]),
        mesh=mesh,
        in_specs=(rows, rows, rows, line, rows, rows, line, line, line) + (P(),) * 12,
        out_specs=(rows, rows),
        check_vma=False,
    )
```

```python
import functools

import jax
import jax.numpy as jnp
from jax import lax
from jax.experimental import pallas as pl
from jax.experimental.pallas import tpu as pltpu
from jax.sharding import PartitionSpec as P

R = 2
EPSILON = 1e-05
L = 128
HALF = 512
WORD_TILE = 3072
GATHER_TILE = 3072
SIZES = (1536, 1536, 1536, 1536)
MESH = pl.DeviceIdType.MESH
F32, BF16, I32, I16 = jnp.float32, jnp.bfloat16, jnp.int32, jnp.int16
UPPER_S, UPPER_R, DEAD = 30, 9, 15
EARLY = 4
PIECES = 2


def offset_list():
    return [number - R if number < R else number - R + 1 for number in range(2 * R)]


def dot(a, b):
    return jnp.dot(a, b, preferred_element_type=F32)


def down(row):
    return jnp.broadcast_to(row, (128, 128)).T


def lanes_from(first):
    return (lax.broadcasted_iota(I32, (16, 128), 1) + first).astype(I16)


def one_hot(column, first, width):
    pieces = []
    for start in range(0, width, 128):
        lanes = jnp.concatenate([lanes_from(first + start)] * (column.shape[0] // 16), axis=0)
        pieces.append(jnp.where(column == lanes, jnp.bfloat16(1), jnp.bfloat16(0)))
    return jnp.concatenate(pieces, axis=1) if len(pieces) > 1 else pieces[0]


def layer_norm(values, gain, bias):
    center = values - jnp.mean(values, axis=-1, keepdims=True)
    spread = jnp.mean(center * center, axis=-1, keepdims=True)
    return center * lax.rsqrt(spread + EPSILON) * gain + bias


def spot_of(step, size):
    return pl.ds(pl.multiple_of(step * size, size), size)


def exchange_kernel(count, old_hbm, ms_hbm, mr_hbm, hs_hbm, xs_hbm, snd_hbm, rcv_hbm, live_hbm, edge_hbm, *rest):
    weights_hbm, rest = rest[:12], rest[12:]
    fresh_ref, far_ref, pre_ref, words_ref, rows_ref, edge_ref = rest[:6]
    weights = rest[6:18]
    (old_ref, ms_ref, mr_ref, hs_ref, xs_ref, snd_ref, rcv_ref, live_ref, send_tab, recv_tab,
     leave_buf, arrive_buf, out_buf, in_buf, stay_buf, new_buf, via_buf, halo_buf, beside_buf, pick_buf, pick_in,
     in_sem, w_sem, lsend, lrecv, hsend, hrecv, bsend, brecv, psend, precv) = rest[18:]
    shifts = offset_list()
    steps = len(shifts)
    loads = [pltpu.make_async_copy(src, dst, in_sem.at[i]) for i, (src, dst) in enumerate([
        (ms_hbm, ms_ref), (old_hbm, old_ref), (mr_hbm, mr_ref), (hs_hbm, hs_ref), (xs_hbm, xs_ref),
        (snd_hbm, snd_ref), (rcv_hbm, rcv_ref), (live_hbm, live_ref), (edge_hbm, edge_ref)])]
    loads += [pltpu.make_async_copy(src, dst, w_sem.at[i]) for i, (src, dst) in enumerate(zip(weights_hbm, weights))]

    arrive_buf[...] = jnp.zeros_like(arrive_buf)
    in_buf[...] = jnp.zeros_like(in_buf)
    beside_buf[...] = jnp.zeros_like(beside_buf)
    pick_in[...] = jnp.zeros_like(pick_in)
    if count:
        me = lax.axis_index("dom")
        other = 1 - lax.axis_index("grp")
        there = [(me + shift >= 0) & (me + shift < count) for shift in shifts]
        peers = [jnp.clip(me + shift, 0, count - 1) for shift in shifts]
        barrier = pltpu.get_barrier_semaphore()
        for peer, real in zip(peers, there):
            @pl.when(real)
            def _():
                pl.semaphore_signal(barrier, inc=1, device_id={"dom": peer}, device_id_type=MESH)
        pl.semaphore_signal(barrier, inc=1, device_id={"grp": other}, device_id_type=MESH)

    for load in loads:
        load.start()
    nodes = old_ref.shape[0]
    moves = ms_ref.shape[1] // steps
    halos = hs_ref.shape[1] // steps
    across = xs_ref.shape[1]
    loads[0].wait()
    want = jnp.concatenate([down(ms_ref[:, i:i + 128]) for i in range(0, ms_ref.shape[1], 128)], axis=0).astype(I16)
    hot = one_hot(want, 0, nodes)
    loads[1].wait()
    old = old_ref[...]
    leave_buf[...] = dot(hot, old).astype(BF16)

    def sends(src, dst, size, send_sem, recv_sem):
        made = []
        for place in range(steps):
            rows = pl.ds(place * size, size)
            made.append(pltpu.make_async_remote_copy(
                src_ref=src.at[rows], dst_ref=dst.at[rows], send_sem=send_sem.at[place], recv_sem=recv_sem.at[place],
                device_id={"dom": peers[place]}, device_id_type=MESH))
        return made

    w1e, w1s, w1r = (weights[0].at[pl.ds(i * L, L)] for i in range(3))
    edges = edge_ref.shape[0]
    subs = WORD_TILE // 128
    ahead_rows, behind_rows = pl.ds(0, 2 * moves), pl.ds(2 * moves, 2 * moves)

    def plan_rows():
        for load in loads[2:5]:
            load.wait()
        take = jnp.concatenate([down(mr_ref[i:i + 1, :]) for i in range(mr_ref.shape[0])], axis=0).astype(I16)
        new_hot = one_hot(take, nodes, arrive_buf.shape[0])
        hwant = jnp.concatenate([down(hs_ref[...]),
                                 down(jnp.concatenate([xs_ref[...]] * (128 // across), axis=1))[:across]],
                                axis=0).astype(I16)
        halo_hot = one_hot(hwant, 0, nodes)
        stay = dot(one_hot(take, 0, nodes), old_ref[...])
        new_buf[...] = new_hot
        via = dot(halo_hot, new_hot).astype(BF16)
        via_buf[...] = via
        pick_buf[0:2 * halos] = via[0:2 * halos, 2 * moves:]
        pick_buf[2 * halos:4 * halos] = via[2 * halos:4 * halos, :2 * moves]
        stay_buf[...] = stay
        halo_buf[...] = dot(halo_hot, stay.astype(BF16))

    def plan_edges():
        for load in loads[5:8]:
            load.wait()
        s, r, live = snd_ref[...], rcv_ref[...], live_ref[...]
        far_s = s >= 2 * HALF
        s_row = jnp.where(far_s, s - HALF, s & (HALF - 1))
        s_up = jnp.where(far_s, 0, s >> 9)
        rows_ref[...] = r & (HALF - 1)
        snd_ref[...] = (s_up << UPPER_S) | (s_row << 16) | ((1 - live) << DEAD) | r
        for load in loads[8:11]:
            load.wait()

        @pl.loop(0, edges // WORD_TILE)
        def _(step):
            spot = spot_of(step, WORD_TILE)
            words_ref[spot] = jnp.concatenate([down(snd_ref[pl.ds(step * subs + i, 1), :]) for i in range(subs)], axis=0)
            pre_ref[spot] = dot(edge_ref[spot], w1e[...]) + weights[1][...]

    def start(copies, conditions):
        for copy, real in zip(copies, conditions):
            pl.when(real)(copy.start)

    def arrived(copies, conditions):
        for copy, real in zip(copies, conditions):
            pl.when(real)(copy.wait_recv)

    if count:
        from_there = [there[steps - 1 - place] for place in range(steps)]
        before_us, after_us = there[R - 1], there[R]
        early = lax.rem(me, 8) < EARLY

        @pl.when(early)
        def _():
            plan_rows()
            plan_edges()

        pl.semaphore_wait(barrier, sum(real.astype(I32) for real in there) + 1)
        first = sends(leave_buf, arrive_buf, moves, lsend, lrecv)
        start(first, there)
        shared = []
        for place in range(steps):
            rows = pl.ds(place * moves, moves)
            shared.append(pltpu.make_async_remote_copy(
                src_ref=leave_buf.at[rows], dst_ref=beside_buf.at[rows],
                send_sem=bsend.at[place], recv_sem=brecv.at[place],
                device_id={"dom": peers[R - 1] if place % 2 == 0 else peers[R]}, device_id_type=MESH))
        shared_to = [before_us, after_us] * R
        shared_from = [after_us, before_us] * R
        start(shared, shared_to)

        @pl.when(jnp.logical_not(early))
        def _():
            plan_rows()

        picks = sends(pick_buf, pick_in, halos, psend, precv)
        start(picks, there)
        second = sends(out_buf, in_buf, halos, hsend, hrecv)
        rows = pl.ds(steps * halos, across)
        swap = pltpu.make_async_remote_copy(
            src_ref=out_buf.at[rows], dst_ref=in_buf.at[rows],
            send_sem=hsend.at[steps], recv_sem=hrecv.at[steps],
            device_id={"grp": other}, device_id_type=MESH)

        arrived(first[R:], from_there[R:])
        slots = pl.ds(2 * halos, 2 * halos)
        out_buf[slots] = (halo_buf[slots] + dot(via_buf[slots, 2 * moves:], arrive_buf[behind_rows])).astype(BF16)
        start(second[R:], there[R:])

        @pl.when(jnp.logical_not(early))
        def _():
            plan_edges()

        arrived(first[:R], from_there[:R])
        slots = pl.ds(0, 2 * halos)
        out_buf[slots] = (halo_buf[slots] + dot(via_buf[slots, :2 * moves], arrive_buf[ahead_rows])).astype(BF16)
        start(second[:R], there[:R])
        out_buf[rows] = (halo_buf[rows] + dot(via_buf[rows], arrive_buf[...])).astype(BF16)
        swap.start()
    else:
        plan_rows()
        plan_edges()
        arrive_buf[...] = leave_buf[...]
        out_buf[...] = (halo_buf[...] + dot(via_buf[...], arrive_buf[...])).astype(BF16)
    for load in loads[11:]:
        load.wait()
    new = arrive_buf[...]

    fresh = (stay_buf[...] + dot(new_buf[...], new)).astype(BF16)
    fresh_ref[...] = fresh
    part = dot(fresh, w1s[...]).astype(BF16)
    send_tab[:, 0:L] = part[:HALF]
    send_tab[:, L:2 * L] = part[HALF:]
    part = dot(fresh, w1r[...]).astype(BF16)
    recv_tab[:, 0:L] = part[:HALF]
    recv_tab[:, L:2 * L] = part[HALF:]

    @pl.loop(0, edges // GATHER_TILE)
    def _(step):
        spot = spot_of(step, GATHER_TILE)
        word = words_ref[spot]
        got_s = dot(one_hot(((word >> 16) & 1023).astype(I16), 0, HALF), send_tab[...])
        got_r = dot(one_hot((word & (HALF - 1)).astype(I16), 0, HALF), recv_tab[...])
        pre_ref[spot] = (pre_ref[spot] + jnp.where((word & (1 << UPPER_S)) != 0, got_s[:, L:], got_s[:, :L])
                         + jnp.where((word & (1 << UPPER_R)) != 0, got_r[:, L:], got_r[:, :L]))

    if count:
        for copies, conditions in ((first, there), (shared, shared_to), (picks, there), (second, there)):
            for copy, real in zip(copies, conditions):
                pl.when(real)(copy.wait_send)
        arrived(shared, shared_from)
        arrived(picks, from_there)
        arrived(second, from_there)
        swap.wait()

        def list_of(buf, place):
            return buf[place * moves:(place + 1) * moves]

        filled = []
        for place, (one, two) in enumerate((((beside_buf, 2), (leave_buf, 3)), ((leave_buf, 2), (beside_buf, 3)),
                                            ((beside_buf, 0), (leave_buf, 1)), ((leave_buf, 0), (beside_buf, 1)))):
            rows = pl.ds(place * halos, halos)
            table = jnp.concatenate([list_of(*one), list_of(*two)], axis=0)
            filled.append((in_buf[rows].astype(F32) + dot(pick_in[rows], table)).astype(BF16))
        halo = jnp.concatenate(filled + [in_buf[pl.ds(steps * halos, across)]], axis=0)
    else:
        halo = out_buf[...]
    far = dot(halo, w1s[...]).astype(BF16)
    far_ref[...] = jnp.concatenate([far, jnp.zeros((far_ref.shape[0] - far.shape[0], L), BF16)], axis=0)


def layer_kernel(fresh_ref, far_ref, pre_ref, words_ref, rows_ref, edge_ref,
                 ew1_ref, eb1_ref, ew2_ref, eb2_ref, eg_ref, eo_ref,
                 nw1_ref, nb1_ref, nw2_ref, nb2_ref, ng_ref, no_ref,
                 node_out, edge_out, new_buf, node_buf, side_0, side_1, sums, out_sem, node_sem):
    tiles = [(sum(SIZES[:i]), size) for i, size in enumerate(SIZES)]
    w2 = ew2_ref[...].astype(F32)
    w2 = (w2 - jnp.mean(w2, axis=-1, keepdims=True)).astype(BF16)
    b2 = eb2_ref[...] - jnp.mean(eb2_ref[...], axis=-1, keepdims=True)
    gain = eg_ref[...] * (L ** 0.5)
    nil = jnp.zeros((L, L), BF16)
    w2_pair = jnp.concatenate([jnp.concatenate([w2, nil], axis=1), jnp.concatenate([nil, w2], axis=1)], axis=0)
    sums[...] = jnp.zeros_like(sums)

    def messages(tile, side):
        first, size = tiles[tile]
        half = size // 2
        spot = pl.ds(first, size)
        word = words_ref[spot]
        far_slot = (word >> 16).astype(I16)
        pair = []
        for i in range(2):
            part = pre_ref[pl.ds(first + i * half, half)]
            part = part + dot(one_hot(far_slot[i * half:(i + 1) * half], HALF, 256), far_ref[...])
            pair.append(jnp.maximum(part.astype(BF16), jnp.bfloat16(0)))
        pair = jnp.concatenate(pair, axis=1)
        center = jnp.concatenate([dot(pair[:half // 2], w2_pair), dot(pair[half // 2:], w2_pair)], axis=0)
        center = jnp.concatenate([center[:, :L], center[:, L:]], axis=0) + b2
        total = jnp.sum(center * center, axis=-1, keepdims=True)
        message = (center * lax.rsqrt(total + EPSILON * L) * gain + eo_ref[...]).astype(BF16)
        code = word.astype(I16)
        zero = jnp.zeros_like(message)
        kept = jnp.where(code >= jnp.int16(0), message, zero)
        new_buf[spot] = edge_ref[spot] + kept
        lower = code < jnp.int16(HALF)
        side[0:size, 0:L] = jnp.where(lower, kept, zero)
        side[0:size, L:2 * L] = jnp.where(lower, zero, kept)

    def save(tile):
        spot = pl.ds(*tiles[tile])
        return pltpu.make_async_copy(new_buf.at[spot], edge_out.at[spot], out_sem.at[tile])

    def gather_in(tile, side):
        first, size = tiles[tile]
        below = lax.broadcasted_iota(I32, (HALF, 128), 0).astype(I16)
        flat = []
        for i in range(first // 128, (first + size) // 128):
            row = jnp.broadcast_to(rows_ref[i:i + 1, :], (16, 128)).astype(I16)
            row = jnp.concatenate([row] * (HALF // 16), axis=0)
            flat.append(jnp.where(row == below, jnp.bfloat16(1), jnp.bfloat16(0)))
        flat = jnp.concatenate(flat, axis=1)
        for i in range(2):
            rows = slice(i * (HALF // 2), (i + 1) * (HALF // 2))
            sums[rows] += dot(flat[rows], side[0:size])

    sides = (side_0, side_1)
    messages(0, side_0)
    for tile in range(len(tiles)):
        if tile + 1 < len(tiles):
            messages(tile + 1, sides[(tile + 1) % 2])
        gather_in(tile, sides[tile % 2])
        save(tile).start()

    fresh = fresh_ref[...]
    inbound = jnp.concatenate([sums[:, :L], sums[:, L:]], axis=0).astype(BF16)
    node_in = jnp.concatenate([fresh, inbound], axis=1)
    piece = fresh.shape[0] // PIECES
    stores = []
    for i in range(PIECES):
        rows = slice(i * piece, (i + 1) * piece)
        hidden = jnp.maximum(dot(node_in[rows], nw1_ref[...]) + nb1_ref[...], 0.0).astype(BF16)
        before = dot(hidden, nw2_ref[...]) + nb2_ref[...]
        node_buf[rows] = (fresh[rows].astype(F32) + layer_norm(before, ng_ref[...], no_ref[...])).astype(BF16)
        stores.append(pltpu.make_async_copy(node_buf.at[pl.ds(i * piece, piece)], node_out.at[pl.ds(i * piece, piece)],
                                            node_sem.at[i]))
        if i:
            stores[i - 1].start()
    stores[-1].start()
    for tile in range(len(tiles)):
        save(tile).wait()
    for store in stores:
        store.wait()


VM = pl.BlockSpec(memory_space=pltpu.VMEM)
ANY = pl.BlockSpec(memory_space=pl.ANY)
HBM = pl.BlockSpec(memory_space=pltpu.HBM)


def in_hbm(x):
    return pltpu.with_memory_space_constraint(x, pltpu.HBM)


def exchange(count, old, mig_send, mig_recv, halo_send, cross_send, lines, edge_latent, vectors):
    nodes, edges = old.shape[0], edge_latent.shape[0]
    far = halo_send.shape[1] + cross_send.shape[1]
    steps = 2 * R
    kept = [((nodes, L), BF16), ((256, L), BF16), ((edges, L), F32), ((edges, L), I32),
            (lines[0].shape, I32), ((edges, L), BF16)] + [(v.shape, v.dtype) for v in vectors]
    operands = [old, mig_send, mig_recv.reshape(-1, 128), halo_send, cross_send, *lines, edge_latent, *vectors]
    params = dict(collective_id=0) if count else {}
    return pl.pallas_call(
        functools.partial(exchange_kernel, count),
        out_shape=tuple(pltpu.VMEM(shape, dtype) for shape, dtype in kept),
        in_specs=[HBM] * len(operands),
        out_specs=(VM,) * len(kept),
        scratch_shapes=[
            pltpu.VMEM(old.shape, BF16), pltpu.VMEM(mig_send.shape, I32), pltpu.VMEM((nodes // 128, 128), I32),
            pltpu.VMEM(halo_send.shape, I32), pltpu.VMEM(cross_send.shape, I32),
            pltpu.VMEM(lines[0].shape, I32), pltpu.VMEM(lines[0].shape, I32), pltpu.VMEM(lines[0].shape, I32),
            pltpu.VMEM((HALF, 2 * L), BF16), pltpu.VMEM((HALF, 2 * L), BF16),
            pltpu.VMEM((mig_send.shape[1], L), BF16), pltpu.VMEM((mig_send.shape[1], L), BF16),
            pltpu.VMEM((far, L), BF16), pltpu.VMEM((far, L), BF16),
            pltpu.VMEM((nodes, L), F32), pltpu.VMEM((nodes, mig_send.shape[1]), BF16),
            pltpu.VMEM((far, mig_send.shape[1]), BF16), pltpu.VMEM((far, L), F32),
            pltpu.VMEM((mig_send.shape[1], L), BF16), pltpu.VMEM((halo_send.shape[1], 128), BF16),
            pltpu.VMEM((halo_send.shape[1], 128), BF16),
            pltpu.SemaphoreType.DMA((9,)), pltpu.SemaphoreType.DMA((len(vectors),)),
            pltpu.SemaphoreType.DMA((steps,)), pltpu.SemaphoreType.DMA((steps,)),
            pltpu.SemaphoreType.DMA((steps + 1,)), pltpu.SemaphoreType.DMA((steps + 1,)),
            *[pltpu.SemaphoreType.DMA((steps,))] * 4,
        ],
        compiler_params=pltpu.CompilerParams(has_side_effects=True, vmem_limit_bytes=24 << 20, **params),
        name="exchange",
    )(*[in_hbm(x) for x in operands])


def layer(parts):
    nodes, edges = parts[0].shape[0], parts[2].shape[0]
    return pl.pallas_call(
        layer_kernel,
        out_shape=(pltpu.HBM((nodes, L), BF16), pltpu.HBM((edges, L), BF16)),
        in_specs=[VM] * len(parts),
        out_specs=(HBM, HBM),
        scratch_shapes=[
            pltpu.VMEM((edges, L), BF16),
            pltpu.VMEM((nodes, L), BF16),
            pltpu.VMEM((max(SIZES), 2 * L), BF16),
            pltpu.VMEM((max(SIZES), 2 * L), BF16),
            pltpu.VMEM((HALF, 2 * L), F32),
            pltpu.SemaphoreType.DMA((len(SIZES),)),
            pltpu.SemaphoreType.DMA((PIECES,)),
        ],
        compiler_params=pltpu.CompilerParams(vmem_limit_bytes=24 << 20),
        name="layer",
    )(*parts)


def step(count, node_latent, edge_latent, mig_send, mig_recv, halo_send, cross_send, senders, receivers, edge_live,
         *weights):
    vectors = [w if w.ndim == 2 else w.reshape(1, -1) for w in weights]
    lines = [v.reshape(-1, 128) for v in (senders, receivers, edge_live)]
    return layer(exchange(count, node_latent, mig_send, mig_recv, halo_send, cross_send, lines, edge_latent, vectors))


def solution(mesh):
    rows, line = P(("grp", "dom"), None), P(("grp", "dom"))
    return jax.shard_map(
        functools.partial(step, mesh.shape["dom"]),
        mesh=mesh,
        in_specs=(rows, rows, rows, line, rows, rows, line, line, line) + (P(),) * 12,
        out_specs=(rows, rows),
        check_vma=False,
    )
```

```python
import functools

import jax
import jax.numpy as jnp
from jax import lax
from jax.experimental import pallas as pl
from jax.experimental.pallas import tpu as pltpu
from jax.sharding import PartitionSpec as P

R = 2
EPSILON = 1e-05
L = 128
HALF = 512
WORD_TILE = 3072
GATHER_TILE = 3072
SIZES = (1536, 1536, 1536, 1536)
MESH = pl.DeviceIdType.MESH
F32, BF16, I32, I16 = jnp.float32, jnp.bfloat16, jnp.int32, jnp.int16
UPPER_S, UPPER_R, DEAD = 30, 9, 15
EARLY = 4
LOCAL_DEEP = False
PIECES = 2


def offset_list():
    return [number - R if number < R else number - R + 1 for number in range(2 * R)]


def dot(a, b):
    return jnp.dot(a, b, preferred_element_type=F32)


def down(row):
    return jnp.broadcast_to(row, (128, 128)).T


def lanes_from(first):
    return (lax.broadcasted_iota(I32, (16, 128), 1) + first).astype(I16)


def one_hot(column, first, width):
    pieces = []
    for start in range(0, width, 128):
        lanes = jnp.concatenate([lanes_from(first + start)] * (column.shape[0] // 16), axis=0)
        pieces.append(jnp.where(column == lanes, jnp.bfloat16(1), jnp.bfloat16(0)))
    return jnp.concatenate(pieces, axis=1) if len(pieces) > 1 else pieces[0]


def layer_norm(values, gain, bias):
    center = values - jnp.mean(values, axis=-1, keepdims=True)
    spread = jnp.mean(center * center, axis=-1, keepdims=True)
    return center * lax.rsqrt(spread + EPSILON) * gain + bias


def spot_of(step, size):
    return pl.ds(pl.multiple_of(step * size, size), size)


def exchange_kernel(count, old_hbm, ms_hbm, mr_hbm, hs_hbm, xs_hbm, snd_hbm, rcv_hbm, live_hbm, edge_hbm, *rest):
    weights_hbm, rest = rest[:12], rest[12:]
    fresh_ref, far_ref, pre_ref, words_ref, rows_ref, edge_ref = rest[:6]
    weights = rest[6:18]
    (old_ref, ms_ref, mr_ref, hs_ref, xs_ref, snd_ref, rcv_ref, live_ref, send_tab, recv_tab,
     leave_buf, arrive_buf, out_buf, in_buf, stay_buf, new_buf, via_buf, halo_buf, beside_buf, pick_buf, pick_in, fill_tab, rank_tab, rank_ref, late_tab,
     in_sem, w_sem, lsend, lrecv, hsend, hrecv, bsend, brecv, psend, precv) = rest[18:]
    shifts = offset_list()
    steps = len(shifts)
    loads = [pltpu.make_async_copy(src, dst, in_sem.at[i]) for i, (src, dst) in enumerate([
        (ms_hbm, ms_ref), (old_hbm, old_ref), (mr_hbm, mr_ref), (hs_hbm, hs_ref), (xs_hbm, xs_ref),
        (snd_hbm, snd_ref), (rcv_hbm, rcv_ref), (live_hbm, live_ref), (edge_hbm, edge_ref)])]
    loads += [pltpu.make_async_copy(src, dst, w_sem.at[i]) for i, (src, dst) in enumerate(zip(weights_hbm, weights))]

    arrive_buf[...] = jnp.zeros_like(arrive_buf)
    in_buf[...] = jnp.zeros_like(in_buf)
    beside_buf[...] = jnp.zeros_like(beside_buf)
    pick_in[...] = jnp.zeros_like(pick_in)
    far_ref[...] = jnp.zeros_like(far_ref)
    if count:
        me = lax.axis_index("dom")
        other = 1 - lax.axis_index("grp")
        there = [(me + shift >= 0) & (me + shift < count) for shift in shifts]
        peers = [jnp.clip(me + shift, 0, count - 1) for shift in shifts]
        barrier = pltpu.get_barrier_semaphore()
        for peer, real in zip(peers, there):
            @pl.when(real)
            def _():
                pl.semaphore_signal(barrier, inc=1, device_id={"dom": peer}, device_id_type=MESH)
        pl.semaphore_signal(barrier, inc=1, device_id={"grp": other}, device_id_type=MESH)

    for load in loads:
        load.start()
    nodes = old_ref.shape[0]
    moves = ms_ref.shape[1] // steps
    halos = hs_ref.shape[1] // steps
    across = xs_ref.shape[1]
    loads[0].wait()
    want = jnp.concatenate([down(ms_ref[:, i:i + 128]) for i in range(0, ms_ref.shape[1], 128)], axis=0).astype(I16)
    hot = one_hot(want, 0, nodes)
    loads[1].wait()
    old = old_ref[...]
    leave_buf[...] = dot(hot, old).astype(BF16)

    def sends(src, dst, size, send_sem, recv_sem):
        made = []
        for place in range(steps):
            rows = pl.ds(place * size, size)
            made.append(pltpu.make_async_remote_copy(
                src_ref=src.at[rows], dst_ref=dst.at[rows], send_sem=send_sem.at[place], recv_sem=recv_sem.at[place],
                device_id={"dom": peers[place]}, device_id_type=MESH))
        return made

    w1e, w1s, w1r = (weights[0].at[pl.ds(i * L, L)] for i in range(3))
    edges = edge_ref.shape[0]
    subs = WORD_TILE // 128
    ahead_rows, behind_rows = pl.ds(0, 2 * moves), pl.ds(2 * moves, 2 * moves)

    def plan_rows():
        for load in loads[2:5]:
            load.wait()
        take = jnp.concatenate([down(mr_ref[i:i + 1, :]) for i in range(mr_ref.shape[0])], axis=0).astype(I16)
        new_hot = one_hot(take, nodes, arrive_buf.shape[0])
        hwant = jnp.concatenate([down(hs_ref[...]),
                                 down(jnp.concatenate([xs_ref[...]] * (128 // across), axis=1))[:across]],
                                axis=0).astype(I16)
        halo_hot = one_hot(hwant, 0, nodes)
        stay = dot(one_hot(take, 0, nodes), old_ref[...])
        new_buf[...] = new_hot
        rank = jnp.where(take >= jnp.int16(nodes), take - jnp.int16(nodes - 1), jnp.int16(0)).astype(F32).astype(BF16)
        rank_tab[:, 0:L] = rank[:HALF]
        rank_tab[:, L:2 * L] = rank[HALF:]
        via = dot(halo_hot, new_hot).astype(BF16)
        via_buf[...] = via
        pick_buf[0:2 * halos] = via[0:2 * halos, 2 * moves:]
        pick_buf[2 * halos:4 * halos] = via[2 * halos:4 * halos, :2 * moves]
        stay_buf[...] = stay
        halo_buf[...] = dot(halo_hot, stay.astype(BF16))

    def plan_edges():
        for load in loads[5:8]:
            load.wait()
        s, r, live = snd_ref[...], rcv_ref[...], live_ref[...]
        far_s = s >= 2 * HALF
        s_row = jnp.where(far_s, s - HALF, s & (HALF - 1))
        s_up = jnp.where(far_s, 0, s >> 9)
        rows_ref[...] = r & (HALF - 1)
        snd_ref[...] = (s_up << UPPER_S) | (s_row << 16) | ((1 - live) << DEAD) | r
        for load in loads[8:11]:
            load.wait()

        @pl.loop(0, edges // WORD_TILE)
        def _(step):
            spot = spot_of(step, WORD_TILE)
            words_ref[spot] = jnp.concatenate([down(snd_ref[pl.ds(step * subs + i, 1), :]) for i in range(subs)], axis=0)
            pre_ref[spot] = dot(edge_ref[spot], w1e[...]) + weights[1][...]

    def project(rows):
        for tab, w in ((send_tab, w1s), (recv_tab, w1r)):
            part = dot(rows, w[...]).astype(BF16)
            tab[:, 0:L] = part[:HALF]
            tab[:, L:2 * L] = part[HALF:]

    def pick_half(word, bit, got):
        return jnp.where((word & (1 << bit)) != 0, got[:, L:], got[:, :L])

    def hot_pair(word):
        return (one_hot(((word >> 16) & 1023).astype(I16), 0, HALF), one_hot((word & (HALF - 1)).astype(I16), 0, HALF))

    def gather_old(step):
        spot = pl.ds(step * GATHER_TILE, GATHER_TILE)
        word = words_ref[spot]
        hot_s, hot_r = hot_pair(word)
        pre_ref[spot] = (pre_ref[spot] + pick_half(word, UPPER_S, dot(hot_s, send_tab[...]))
                         + pick_half(word, UPPER_R, dot(hot_r, recv_tab[...])))
        rank_s = pick_half(word, UPPER_S, dot(hot_s, rank_tab[...])).astype(I32)
        rank_r = pick_half(word, UPPER_R, dot(hot_r, rank_tab[...])).astype(I32)
        rank_ref[spot] = (rank_r << 16) | rank_s

    def gather_new():
        late_tab[0:steps * moves] = dot(arrive_buf[...], w1s[...]).astype(BF16)
        late_tab[steps * moves:] = dot(arrive_buf[...], w1r[...]).astype(BF16)

        @pl.loop(0, edges // GATHER_TILE)
        def _(step):
            spot = spot_of(step, GATHER_TILE)
            word = rank_ref[spot]
            hot = jnp.concatenate([one_hot(word.astype(I16), 1, steps * moves),
                                   one_hot((word >> 16).astype(I16), 1, steps * moves)], axis=1)
            mid = GATHER_TILE // 2
            pre_ref[spot] = pre_ref[spot] + jnp.concatenate([dot(hot[:mid], late_tab[...]), dot(hot[mid:], late_tab[...])],
                                                            axis=0)

    def gather_all(fresh):
        project(fresh)

        @pl.loop(0, edges // GATHER_TILE)
        def _(step):
            spot = spot_of(step, GATHER_TILE)
            word = words_ref[spot]
            hot_s, hot_r = hot_pair(word)
            pre_ref[spot] = (pre_ref[spot] + pick_half(word, UPPER_S, dot(hot_s, send_tab[...]))
                             + pick_half(word, UPPER_R, dot(hot_r, recv_tab[...])))

    def start(copies, conditions):
        for copy, real in zip(copies, conditions):
            pl.when(real)(copy.start)

    def arrived(copies, conditions):
        for copy, real in zip(copies, conditions):
            pl.when(real)(copy.wait_recv)

    if count:
        from_there = [there[steps - 1 - place] for place in range(steps)]
        before_us, after_us = there[R - 1], there[R]
        early = lax.rem(me, 8) < EARLY

        @pl.when(early)
        def _():
            plan_rows()
            plan_edges()

        deep = (lax.rem(me, 32) < 2) & (me >= 32)

        @pl.when(deep)
        def _():
            project(stay_buf[...].astype(BF16))
            gather_old(0)

        pl.semaphore_wait(barrier, sum(real.astype(I32) for real in there) + 1)
        first = sends(leave_buf, arrive_buf, moves, lsend, lrecv)
        start(first, there)
        shared = []
        for place in range(steps):
            rows = pl.ds(place * moves, moves)
            shared.append(pltpu.make_async_remote_copy(
                src_ref=leave_buf.at[rows], dst_ref=beside_buf.at[rows],
                send_sem=bsend.at[place], recv_sem=brecv.at[place],
                device_id={"dom": peers[R - 1] if place % 2 == 0 else peers[R]}, device_id_type=MESH))
        shared_to = [before_us, after_us] * R
        shared_from = [after_us, before_us] * R
        start(shared, shared_to)

        @pl.when(jnp.logical_not(early))
        def _():
            plan_rows()

        picks = sends(pick_buf, pick_in, halos, psend, precv)
        start(picks, there)

        @pl.when(deep)
        def _():
            for step in range(1, edges // GATHER_TILE):
                gather_old(step)

        second = sends(out_buf, in_buf, halos, hsend, hrecv)
        rows = pl.ds(steps * halos, across)
        swap = pltpu.make_async_remote_copy(
            src_ref=out_buf.at[rows], dst_ref=in_buf.at[rows],
            send_sem=hsend.at[steps], recv_sem=hrecv.at[steps],
            device_id={"grp": other}, device_id_type=MESH)

        def send_ahead():
            arrived(first[R:], from_there[R:])
            slots = pl.ds(2 * halos, 2 * halos)
            out_buf[slots] = (halo_buf[slots] + dot(via_buf[slots, 2 * moves:], arrive_buf[behind_rows])).astype(BF16)
            start(second[R:], there[R:])

        def send_behind():
            arrived(first[:R], from_there[:R])
            slots = pl.ds(0, 2 * halos)
            out_buf[slots] = (halo_buf[slots] + dot(via_buf[slots, :2 * moves], arrive_buf[ahead_rows])).astype(BF16)
            start(second[:R], there[:R])

        @pl.when(early)
        def _():
            send_behind()
            send_ahead()

        @pl.when(jnp.logical_not(early))
        def _():
            send_ahead()
            plan_edges()
            send_behind()

        out_buf[rows] = (halo_buf[rows] + dot(via_buf[rows], arrive_buf[...])).astype(BF16)
        swap.start()
    else:
        plan_rows()
        plan_edges()
        if LOCAL_DEEP:
            project(stay_buf[...].astype(BF16))
            for step in range(edges // GATHER_TILE):
                gather_old(step)
        arrive_buf[...] = leave_buf[...]
        out_buf[...] = (halo_buf[...] + dot(via_buf[...], arrive_buf[...])).astype(BF16)
    for load in loads[11:]:
        load.wait()
    new = arrive_buf[...]

    fresh = (stay_buf[...] + dot(new_buf[...], new)).astype(BF16)
    fresh_ref[...] = fresh
    if count:
        arrived(shared, shared_from)

        def list_of(buf, place):
            return buf[place * moves:(place + 1) * moves]

        for place, (one, two) in enumerate((((beside_buf, 2), (leave_buf, 3)), ((leave_buf, 2), (beside_buf, 3)),
                                            ((beside_buf, 0), (leave_buf, 1)), ((leave_buf, 0), (beside_buf, 1)))):
            table = jnp.concatenate([list_of(*one), list_of(*two)], axis=0)
            fill_tab[place, 0:L] = w1s[...]
            fill_tab[place, L:2 * L] = dot(table, w1s[...]).astype(BF16)

    if count:
        pl.when(deep)(gather_new)
        pl.when(jnp.logical_not(deep))(lambda: gather_all(fresh_ref[...]))
    elif LOCAL_DEEP:
        gather_new()
    else:
        gather_all(fresh)

    tail = pl.ds(steps * halos, across)
    if count:
        arrived(picks, from_there)
        arrived(second, from_there)
        swap.wait_recv()
        for place in range(steps):
            rows = pl.ds(place * halos, halos)
            far_ref[rows] = dot(jnp.concatenate([in_buf[rows], pick_in[rows]], axis=1), fill_tab[place]).astype(BF16)
        far_ref[tail] = dot(in_buf[tail], w1s[...]).astype(BF16)
        swap.wait_send()
        for copies, conditions in ((first, there), (shared, shared_to), (picks, there), (second, there)):
            for copy, real in zip(copies, conditions):
                pl.when(real)(copy.wait_send)
    else:
        far_ref[pl.ds(0, steps * halos + across)] = dot(out_buf[...], w1s[...]).astype(BF16)


def layer_kernel(fresh_ref, far_ref, pre_ref, words_ref, rows_ref, edge_ref,
                 ew1_ref, eb1_ref, ew2_ref, eb2_ref, eg_ref, eo_ref,
                 nw1_ref, nb1_ref, nw2_ref, nb2_ref, ng_ref, no_ref,
                 node_out, edge_out, new_buf, node_buf, side_0, side_1, sums, out_sem, node_sem):
    tiles = [(sum(SIZES[:i]), size) for i, size in enumerate(SIZES)]
    w2 = ew2_ref[...].astype(F32)
    w2 = (w2 - jnp.mean(w2, axis=-1, keepdims=True)).astype(BF16)
    b2 = eb2_ref[...] - jnp.mean(eb2_ref[...], axis=-1, keepdims=True)
    gain = eg_ref[...] * (L ** 0.5)
    nil = jnp.zeros((L, L), BF16)
    w2_pair = jnp.concatenate([jnp.concatenate([w2, nil], axis=1), jnp.concatenate([nil, w2], axis=1)], axis=0)
    sums[...] = jnp.zeros_like(sums)

    def messages(tile, side):
        first, size = tiles[tile]
        half = size // 2
        spot = pl.ds(first, size)
        word = words_ref[spot]
        far_slot = (word >> 16).astype(I16)
        pair = []
        for i in range(2):
            part = pre_ref[pl.ds(first + i * half, half)]
            part = part + dot(one_hot(far_slot[i * half:(i + 1) * half], HALF, 256), far_ref[...])
            pair.append(jnp.maximum(part.astype(BF16), jnp.bfloat16(0)))
        pair = jnp.concatenate(pair, axis=1)
        center = jnp.concatenate([dot(pair[:half // 2], w2_pair), dot(pair[half // 2:], w2_pair)], axis=0)
        center = jnp.concatenate([center[:, :L], center[:, L:]], axis=0) + b2
        total = jnp.sum(center * center, axis=-1, keepdims=True)
        message = (center * lax.rsqrt(total + EPSILON * L) * gain + eo_ref[...]).astype(BF16)
        code = word.astype(I16)
        zero = jnp.zeros_like(message)
        kept = jnp.where(code >= jnp.int16(0), message, zero)
        new_buf[spot] = edge_ref[spot] + kept
        lower = code < jnp.int16(HALF)
        side[0:size, 0:L] = jnp.where(lower, kept, zero)
        side[0:size, L:2 * L] = jnp.where(lower, zero, kept)

    def save(tile):
        spot = pl.ds(*tiles[tile])
        return pltpu.make_async_copy(new_buf.at[spot], edge_out.at[spot], out_sem.at[tile])

    def gather_in(tile, side):
        first, size = tiles[tile]
        below = lax.broadcasted_iota(I32, (HALF, 128), 0).astype(I16)
        flat = []
        for i in range(first // 128, (first + size) // 128):
            row = jnp.broadcast_to(rows_ref[i:i + 1, :], (16, 128)).astype(I16)
            row = jnp.concatenate([row] * (HALF // 16), axis=0)
            flat.append(jnp.where(row == below, jnp.bfloat16(1), jnp.bfloat16(0)))
        flat = jnp.concatenate(flat, axis=1)
        for i in range(2):
            rows = slice(i * (HALF // 2), (i + 1) * (HALF // 2))
            sums[rows] += dot(flat[rows], side[0:size])

    sides = (side_0, side_1)
    messages(0, side_0)
    for tile in range(len(tiles)):
        if tile + 1 < len(tiles):
            messages(tile + 1, sides[(tile + 1) % 2])
        gather_in(tile, sides[tile % 2])
        save(tile).start()

    fresh = fresh_ref[...]
    inbound = jnp.concatenate([sums[:, :L], sums[:, L:]], axis=0).astype(BF16)
    node_in = jnp.concatenate([fresh, inbound], axis=1)
    piece = fresh.shape[0] // PIECES
    stores = []
    for i in range(PIECES):
        rows = slice(i * piece, (i + 1) * piece)
        hidden = jnp.maximum(dot(node_in[rows], nw1_ref[...]) + nb1_ref[...], 0.0).astype(BF16)
        before = dot(hidden, nw2_ref[...]) + nb2_ref[...]
        node_buf[rows] = (fresh[rows].astype(F32) + layer_norm(before, ng_ref[...], no_ref[...])).astype(BF16)
        stores.append(pltpu.make_async_copy(node_buf.at[pl.ds(i * piece, piece)], node_out.at[pl.ds(i * piece, piece)],
                                            node_sem.at[i]))
        if i:
            stores[i - 1].start()
    stores[-1].start()
    for tile in range(len(tiles)):
        save(tile).wait()
    for store in stores:
        store.wait()


VM = pl.BlockSpec(memory_space=pltpu.VMEM)
ANY = pl.BlockSpec(memory_space=pl.ANY)
HBM = pl.BlockSpec(memory_space=pltpu.HBM)


def in_hbm(x):
    return pltpu.with_memory_space_constraint(x, pltpu.HBM)


def exchange(count, old, mig_send, mig_recv, halo_send, cross_send, lines, edge_latent, vectors):
    nodes, edges = old.shape[0], edge_latent.shape[0]
    far = halo_send.shape[1] + cross_send.shape[1]
    steps = 2 * R
    kept = [((nodes, L), BF16), ((256, L), BF16), ((edges, L), F32), ((edges, L), I32),
            (lines[0].shape, I32), ((edges, L), BF16)] + [(v.shape, v.dtype) for v in vectors]
    operands = [old, mig_send, mig_recv.reshape(-1, 128), halo_send, cross_send, *lines, edge_latent, *vectors]
    params = dict(collective_id=0) if count else {}
    return pl.pallas_call(
        functools.partial(exchange_kernel, count),
        out_shape=tuple(pltpu.VMEM(shape, dtype) for shape, dtype in kept),
        in_specs=[HBM] * len(operands),
        out_specs=(VM,) * len(kept),
        scratch_shapes=[
            pltpu.VMEM(old.shape, BF16), pltpu.VMEM(mig_send.shape, I32), pltpu.VMEM((nodes // 128, 128), I32),
            pltpu.VMEM(halo_send.shape, I32), pltpu.VMEM(cross_send.shape, I32),
            pltpu.VMEM(lines[0].shape, I32), pltpu.VMEM(lines[0].shape, I32), pltpu.VMEM(lines[0].shape, I32),
            pltpu.VMEM((HALF, 2 * L), BF16), pltpu.VMEM((HALF, 2 * L), BF16),
            pltpu.VMEM((mig_send.shape[1], L), BF16), pltpu.VMEM((mig_send.shape[1], L), BF16),
            pltpu.VMEM((far, L), BF16), pltpu.VMEM((far, L), BF16),
            pltpu.VMEM((nodes, L), F32), pltpu.VMEM((nodes, mig_send.shape[1]), BF16),
            pltpu.VMEM((far, mig_send.shape[1]), BF16), pltpu.VMEM((far, L), F32),
            pltpu.VMEM((mig_send.shape[1], L), BF16), pltpu.VMEM((halo_send.shape[1], 128), BF16),
            pltpu.VMEM((halo_send.shape[1], 128), BF16),
            pltpu.VMEM((steps, 2 * L, L), BF16), pltpu.VMEM((HALF, 2 * L), BF16), pltpu.VMEM((edges, L), I32),
            pltpu.VMEM((2 * mig_send.shape[1], L), BF16),
            pltpu.SemaphoreType.DMA((9,)), pltpu.SemaphoreType.DMA((len(vectors),)),
            pltpu.SemaphoreType.DMA((steps,)), pltpu.SemaphoreType.DMA((steps,)),
            pltpu.SemaphoreType.DMA((steps + 1,)), pltpu.SemaphoreType.DMA((steps + 1,)),
            *[pltpu.SemaphoreType.DMA((steps,))] * 4,
        ],
        compiler_params=pltpu.CompilerParams(has_side_effects=True, vmem_limit_bytes=24 << 20, **params),
        name="exchange",
    )(*[in_hbm(x) for x in operands])


def layer(parts):
    nodes, edges = parts[0].shape[0], parts[2].shape[0]
    return pl.pallas_call(
        layer_kernel,
        out_shape=(pltpu.HBM((nodes, L), BF16), pltpu.HBM((edges, L), BF16)),
        in_specs=[VM] * len(parts),
        out_specs=(HBM, HBM),
        scratch_shapes=[
            pltpu.VMEM((edges, L), BF16),
            pltpu.VMEM((nodes, L), BF16),
            pltpu.VMEM((max(SIZES), 2 * L), BF16),
            pltpu.VMEM((max(SIZES), 2 * L), BF16),
            pltpu.VMEM((HALF, 2 * L), F32),
            pltpu.SemaphoreType.DMA((len(SIZES),)),
            pltpu.SemaphoreType.DMA((PIECES,)),
        ],
        compiler_params=pltpu.CompilerParams(vmem_limit_bytes=24 << 20),
        name="layer",
    )(*parts)


def step(count, node_latent, edge_latent, mig_send, mig_recv, halo_send, cross_send, senders, receivers, edge_live,
         *weights):
    vectors = [w if w.ndim == 2 else w.reshape(1, -1) for w in weights]
    lines = [v.reshape(-1, 128) for v in (senders, receivers, edge_live)]
    return layer(exchange(count, node_latent, mig_send, mig_recv, halo_send, cross_send, lines, edge_latent, vectors))


def solution(mesh):
    rows, line = P(("grp", "dom"), None), P(("grp", "dom"))
    return jax.shard_map(
        functools.partial(step, mesh.shape["dom"]),
        mesh=mesh,
        in_specs=(rows, rows, rows, line, rows, rows, line, line, line) + (P(),) * 12,
        out_specs=(rows, rows),
        check_vma=False,
    )
```

```python
import functools

import jax
import jax.numpy as jnp
from jax import lax
from jax.experimental import pallas as pl
from jax.experimental.pallas import tpu as pltpu
from jax.sharding import PartitionSpec as P

R = 2
EPSILON = 1e-05
L = 128
HALF = 512
WORD_TILE = 3072
GATHER_TILE = 3072
SIZES = (1536, 1536, 1536, 1536)
MESH = pl.DeviceIdType.MESH
F32, BF16, I32, I16 = jnp.float32, jnp.bfloat16, jnp.int32, jnp.int16
UPPER_S, UPPER_R, DEAD = 30, 9, 15
EARLY = 4
LOCAL_DEEP = False
PIECES = 2


def offset_list():
    return [number - R if number < R else number - R + 1 for number in range(2 * R)]


def dot(a, b):
    return jnp.dot(a, b, preferred_element_type=F32)


def down(row):
    return jnp.broadcast_to(row, (128, 128)).T


def lanes_from(first):
    return (lax.broadcasted_iota(I32, (16, 128), 1) + first).astype(I16)


def one_hot(column, first, width):
    pieces = []
    for start in range(0, width, 128):
        lanes = jnp.concatenate([lanes_from(first + start)] * (column.shape[0] // 16), axis=0)
        pieces.append(jnp.where(column == lanes, jnp.bfloat16(1), jnp.bfloat16(0)))
    return jnp.concatenate(pieces, axis=1) if len(pieces) > 1 else pieces[0]


def layer_norm(values, gain, bias):
    center = values - jnp.mean(values, axis=-1, keepdims=True)
    spread = jnp.mean(center * center, axis=-1, keepdims=True)
    return center * lax.rsqrt(spread + EPSILON) * gain + bias


def spot_of(step, size):
    return pl.ds(pl.multiple_of(step * size, size), size)


def exchange_kernel(count, old_hbm, ms_hbm, mr_hbm, hs_hbm, xs_hbm, snd_hbm, rcv_hbm, live_hbm, edge_hbm, *rest):
    weights_hbm, rest = rest[:12], rest[12:]
    fresh_ref, far_ref, pre_ref, words_ref, rows_ref, edge_ref = rest[:6]
    weights = rest[6:18]
    (old_ref, ms_ref, mr_ref, hs_ref, xs_ref, snd_ref, rcv_ref, live_ref, send_tab, recv_tab,
     leave_buf, arrive_buf, out_buf, in_buf, stay_buf, new_buf, via_buf, halo_buf, beside_buf, pick_buf, pick_in, fill_tab, rank_tab, rank_ref, late_tab,
     in_sem, w_sem, lsend, lrecv, hsend, hrecv, bsend, brecv, psend, precv) = rest[18:]
    shifts = offset_list()
    steps = len(shifts)
    loads = [pltpu.make_async_copy(src, dst, in_sem.at[i]) for i, (src, dst) in enumerate([
        (ms_hbm, ms_ref), (old_hbm, old_ref), (mr_hbm, mr_ref), (hs_hbm, hs_ref), (xs_hbm, xs_ref),
        (snd_hbm, snd_ref), (rcv_hbm, rcv_ref), (live_hbm, live_ref), (edge_hbm, edge_ref)])]
    loads += [pltpu.make_async_copy(src, dst, w_sem.at[i]) for i, (src, dst) in enumerate(zip(weights_hbm, weights))]

    arrive_buf[...] = jnp.zeros_like(arrive_buf)
    in_buf[...] = jnp.zeros_like(in_buf)
    beside_buf[...] = jnp.zeros_like(beside_buf)
    pick_in[...] = jnp.zeros_like(pick_in)
    far_ref[...] = jnp.zeros_like(far_ref)
    if count:
        me = lax.axis_index("dom")
        other = 1 - lax.axis_index("grp")
        there = [(me + shift >= 0) & (me + shift < count) for shift in shifts]
        peers = [jnp.clip(me + shift, 0, count - 1) for shift in shifts]
        barrier = pltpu.get_barrier_semaphore()
        for peer, real in zip(peers, there):
            @pl.when(real)
            def _():
                pl.semaphore_signal(barrier, inc=1, device_id={"dom": peer}, device_id_type=MESH)
        pl.semaphore_signal(barrier, inc=1, device_id={"grp": other}, device_id_type=MESH)

    for load in loads:
        load.start()
    nodes = old_ref.shape[0]
    moves = ms_ref.shape[1] // steps
    halos = hs_ref.shape[1] // steps
    across = xs_ref.shape[1]
    loads[0].wait()
    want = jnp.concatenate([down(ms_ref[:, i:i + 128]) for i in range(0, ms_ref.shape[1], 128)], axis=0).astype(I16)
    hot = one_hot(want, 0, nodes)
    loads[1].wait()
    old = old_ref[...]
    leave_buf[...] = dot(hot, old).astype(BF16)

    def sends(src, dst, size, send_sem, recv_sem):
        made = []
        for place in range(steps):
            rows = pl.ds(place * size, size)
            made.append(pltpu.make_async_remote_copy(
                src_ref=src.at[rows], dst_ref=dst.at[rows], send_sem=send_sem.at[place], recv_sem=recv_sem.at[place],
                device_id={"dom": peers[place]}, device_id_type=MESH))
        return made

    w1e, w1s, w1r = (weights[0].at[pl.ds(i * L, L)] for i in range(3))
    edges = edge_ref.shape[0]
    subs = WORD_TILE // 128
    ahead_rows, behind_rows = pl.ds(0, 2 * moves), pl.ds(2 * moves, 2 * moves)

    def plan_rows():
        for load in loads[2:5]:
            load.wait()
        take = jnp.concatenate([down(mr_ref[i:i + 1, :]) for i in range(mr_ref.shape[0])], axis=0).astype(I16)
        new_hot = one_hot(take, nodes, arrive_buf.shape[0])
        hwant = jnp.concatenate([down(hs_ref[...]),
                                 down(jnp.concatenate([xs_ref[...]] * (128 // across), axis=1))[:across]],
                                axis=0).astype(I16)
        halo_hot = one_hot(hwant, 0, nodes)
        stay = dot(one_hot(take, 0, nodes), old_ref[...])
        new_buf[...] = new_hot
        rank = jnp.where(take >= jnp.int16(nodes), take - jnp.int16(nodes - 1), jnp.int16(0)).astype(F32).astype(BF16)
        rank_tab[:, 0:L] = rank[:HALF]
        rank_tab[:, L:2 * L] = rank[HALF:]
        via = dot(halo_hot, new_hot).astype(BF16)
        via_buf[...] = via
        pick_buf[0:2 * halos] = via[0:2 * halos, 2 * moves:]
        pick_buf[2 * halos:4 * halos] = via[2 * halos:4 * halos, :2 * moves]
        stay_buf[...] = stay
        halo_buf[...] = dot(halo_hot, stay.astype(BF16))

    def plan_edges():
        for load in loads[5:8]:
            load.wait()
        s, r, live = snd_ref[...], rcv_ref[...], live_ref[...]
        far_s = s >= 2 * HALF
        s_row = jnp.where(far_s, s - HALF, s & (HALF - 1))
        s_up = jnp.where(far_s, 0, s >> 9)
        rows_ref[...] = r & (HALF - 1)
        snd_ref[...] = (s_up << UPPER_S) | (s_row << 16) | ((1 - live) << DEAD) | r
        for load in loads[8:11]:
            load.wait()

        @pl.loop(0, edges // WORD_TILE)
        def _(step):
            spot = spot_of(step, WORD_TILE)
            words_ref[spot] = jnp.concatenate([down(snd_ref[pl.ds(step * subs + i, 1), :]) for i in range(subs)], axis=0)
            pre_ref[spot] = dot(edge_ref[spot], w1e[...]) + weights[1][...]

    def project(rows):
        for tab, w in ((send_tab, w1s), (recv_tab, w1r)):
            part = dot(rows, w[...]).astype(BF16)
            tab[:, 0:L] = part[:HALF]
            tab[:, L:2 * L] = part[HALF:]

    def pick_half(word, bit, got):
        return jnp.where((word & (1 << bit)) != 0, got[:, L:], got[:, :L])

    def hot_pair(word):
        return (one_hot(((word >> 16) & 1023).astype(I16), 0, HALF), one_hot((word & (HALF - 1)).astype(I16), 0, HALF))

    def gather_old(step):
        spot = pl.ds(step * GATHER_TILE, GATHER_TILE)
        word = words_ref[spot]
        hot_s, hot_r = hot_pair(word)
        pre_ref[spot] = (pre_ref[spot] + pick_half(word, UPPER_S, dot(hot_s, send_tab[...]))
                         + pick_half(word, UPPER_R, dot(hot_r, recv_tab[...])))
        rank_s = pick_half(word, UPPER_S, dot(hot_s, rank_tab[...])).astype(I32)
        rank_r = pick_half(word, UPPER_R, dot(hot_r, rank_tab[...])).astype(I32)
        rank_ref[spot] = (rank_r << 16) | rank_s

    def gather_new():
        late_tab[0:steps * moves] = dot(arrive_buf[...], w1s[...]).astype(BF16)
        late_tab[steps * moves:] = dot(arrive_buf[...], w1r[...]).astype(BF16)

        @pl.loop(0, edges // GATHER_TILE)
        def _(step):
            spot = spot_of(step, GATHER_TILE)
            word = rank_ref[spot]
            hot = jnp.concatenate([one_hot(word.astype(I16), 1, steps * moves),
                                   one_hot((word >> 16).astype(I16), 1, steps * moves)], axis=1)
            mid = GATHER_TILE // 2
            pre_ref[spot] = pre_ref[spot] + jnp.concatenate([dot(hot[:mid], late_tab[...]), dot(hot[mid:], late_tab[...])],
                                                            axis=0)

    def gather_all(fresh):
        project(fresh)

        @pl.loop(0, edges // GATHER_TILE)
        def _(step):
            spot = spot_of(step, GATHER_TILE)
            word = words_ref[spot]
            hot_s, hot_r = hot_pair(word)
            pre_ref[spot] = (pre_ref[spot] + pick_half(word, UPPER_S, dot(hot_s, send_tab[...]))
                             + pick_half(word, UPPER_R, dot(hot_r, recv_tab[...])))

    def start(copies, conditions):
        for copy, real in zip(copies, conditions):
            pl.when(real)(copy.start)

    def arrived(copies, conditions):
        for copy, real in zip(copies, conditions):
            pl.when(real)(copy.wait_recv)

    if count:
        from_there = [there[steps - 1 - place] for place in range(steps)]
        before_us, after_us = there[R - 1], there[R]
        early = lax.rem(me, 8) < EARLY

        @pl.when(early)
        def _():
            plan_rows()
            plan_edges()

        deep = (lax.rem(me, 8) < 2) & (me >= 8)

        @pl.when(deep)
        def _():
            project(stay_buf[...].astype(BF16))
            gather_old(0)

        pl.semaphore_wait(barrier, sum(real.astype(I32) for real in there) + 1)
        first = sends(leave_buf, arrive_buf, moves, lsend, lrecv)
        start(first, there)
        shared = []
        for place in range(steps):
            rows = pl.ds(place * moves, moves)
            shared.append(pltpu.make_async_remote_copy(
                src_ref=leave_buf.at[rows], dst_ref=beside_buf.at[rows],
                send_sem=bsend.at[place], recv_sem=brecv.at[place],
                device_id={"dom": peers[R - 1] if place % 2 == 0 else peers[R]}, device_id_type=MESH))
        shared_to = [before_us, after_us] * R
        shared_from = [after_us, before_us] * R
        start(shared, shared_to)

        @pl.when(jnp.logical_not(early))
        def _():
            plan_rows()

        picks = sends(pick_buf, pick_in, halos, psend, precv)
        start(picks, there)

        @pl.when(deep)
        def _():
            for step in range(1, edges // GATHER_TILE):
                gather_old(step)

        second = sends(out_buf, in_buf, halos, hsend, hrecv)
        rows = pl.ds(steps * halos, across)
        swap = pltpu.make_async_remote_copy(
            src_ref=out_buf.at[rows], dst_ref=in_buf.at[rows],
            send_sem=hsend.at[steps], recv_sem=hrecv.at[steps],
            device_id={"grp": other}, device_id_type=MESH)

        def send_ahead():
            arrived(first[R:], from_there[R:])
            slots = pl.ds(2 * halos, 2 * halos)
            out_buf[slots] = (halo_buf[slots] + dot(via_buf[slots, 2 * moves:], arrive_buf[behind_rows])).astype(BF16)
            start(second[R:], there[R:])

        def send_behind():
            arrived(first[:R], from_there[:R])
            slots = pl.ds(0, 2 * halos)
            out_buf[slots] = (halo_buf[slots] + dot(via_buf[slots, :2 * moves], arrive_buf[ahead_rows])).astype(BF16)
            start(second[:R], there[:R])

        @pl.when(early)
        def _():
            send_behind()
            send_ahead()

        @pl.when(jnp.logical_not(early))
        def _():
            send_ahead()
            plan_edges()
            send_behind()

        out_buf[rows] = (halo_buf[rows] + dot(via_buf[rows], arrive_buf[...])).astype(BF16)
        swap.start()
    else:
        plan_rows()
        plan_edges()
        if LOCAL_DEEP:
            project(stay_buf[...].astype(BF16))
            for step in range(edges // GATHER_TILE):
                gather_old(step)
        arrive_buf[...] = leave_buf[...]
        out_buf[...] = (halo_buf[...] + dot(via_buf[...], arrive_buf[...])).astype(BF16)
    for load in loads[11:]:
        load.wait()
    new = arrive_buf[...]

    fresh = (stay_buf[...] + dot(new_buf[...], new)).astype(BF16)
    fresh_ref[...] = fresh
    if count:
        arrived(shared, shared_from)

        def list_of(buf, place):
            return buf[place * moves:(place + 1) * moves]

        for place, (one, two) in enumerate((((beside_buf, 2), (leave_buf, 3)), ((leave_buf, 2), (beside_buf, 3)),
                                            ((beside_buf, 0), (leave_buf, 1)), ((leave_buf, 0), (beside_buf, 1)))):
            table = jnp.concatenate([list_of(*one), list_of(*two)], axis=0)
            fill_tab[place, 0:L] = w1s[...]
            fill_tab[place, L:2 * L] = dot(table, w1s[...]).astype(BF16)

    if count:
        pl.when(deep)(gather_new)
        pl.when(jnp.logical_not(deep))(lambda: gather_all(fresh_ref[...]))
    elif LOCAL_DEEP:
        gather_new()
    else:
        gather_all(fresh)

    tail = pl.ds(steps * halos, across)
    if count:
        arrived(picks, from_there)
        arrived(second, from_there)
        swap.wait_recv()
        for place in range(steps):
            rows = pl.ds(place * halos, halos)
            far_ref[rows] = dot(jnp.concatenate([in_buf[rows], pick_in[rows]], axis=1), fill_tab[place]).astype(BF16)
        far_ref[tail] = dot(in_buf[tail], w1s[...]).astype(BF16)
        swap.wait_send()
        for copies, conditions in ((first, there), (shared, shared_to), (picks, there), (second, there)):
            for copy, real in zip(copies, conditions):
                pl.when(real)(copy.wait_send)
    else:
        far_ref[pl.ds(0, steps * halos + across)] = dot(out_buf[...], w1s[...]).astype(BF16)


def layer_kernel(fresh_ref, far_ref, pre_ref, words_ref, rows_ref, edge_ref,
                 ew1_ref, eb1_ref, ew2_ref, eb2_ref, eg_ref, eo_ref,
                 nw1_ref, nb1_ref, nw2_ref, nb2_ref, ng_ref, no_ref,
                 node_out, edge_out, new_buf, node_buf, side_0, side_1, sums, out_sem, node_sem):
    tiles = [(sum(SIZES[:i]), size) for i, size in enumerate(SIZES)]
    w2 = ew2_ref[...].astype(F32)
    w2 = (w2 - jnp.mean(w2, axis=-1, keepdims=True)).astype(BF16)
    b2 = eb2_ref[...] - jnp.mean(eb2_ref[...], axis=-1, keepdims=True)
    gain = eg_ref[...] * (L ** 0.5)
    nil = jnp.zeros((L, L), BF16)
    w2_pair = jnp.concatenate([jnp.concatenate([w2, nil], axis=1), jnp.concatenate([nil, w2], axis=1)], axis=0)
    sums[...] = jnp.zeros_like(sums)

    def messages(tile, side):
        first, size = tiles[tile]
        half = size // 2
        spot = pl.ds(first, size)
        word = words_ref[spot]
        far_slot = (word >> 16).astype(I16)
        pair = []
        for i in range(2):
            part = pre_ref[pl.ds(first + i * half, half)]
            part = part + dot(one_hot(far_slot[i * half:(i + 1) * half], HALF, 256), far_ref[...])
            pair.append(jnp.maximum(part.astype(BF16), jnp.bfloat16(0)))
        pair = jnp.concatenate(pair, axis=1)
        center = jnp.concatenate([dot(pair[:half // 2], w2_pair), dot(pair[half // 2:], w2_pair)], axis=0)
        center = jnp.concatenate([center[:, :L], center[:, L:]], axis=0) + b2
        total = jnp.sum(center * center, axis=-1, keepdims=True)
        message = (center * lax.rsqrt(total + EPSILON * L) * gain + eo_ref[...]).astype(BF16)
        code = word.astype(I16)
        zero = jnp.zeros_like(message)
        kept = jnp.where(code >= jnp.int16(0), message, zero)
        new_buf[spot] = edge_ref[spot] + kept
        lower = code < jnp.int16(HALF)
        side[0:size, 0:L] = jnp.where(lower, kept, zero)
        side[0:size, L:2 * L] = jnp.where(lower, zero, kept)

    def save(tile):
        spot = pl.ds(*tiles[tile])
        return pltpu.make_async_copy(new_buf.at[spot], edge_out.at[spot], out_sem.at[tile])

    def gather_in(tile, side):
        first, size = tiles[tile]
        below = lax.broadcasted_iota(I32, (HALF, 128), 0).astype(I16)
        flat = []
        for i in range(first // 128, (first + size) // 128):
            row = jnp.broadcast_to(rows_ref[i:i + 1, :], (16, 128)).astype(I16)
            row = jnp.concatenate([row] * (HALF // 16), axis=0)
            flat.append(jnp.where(row == below, jnp.bfloat16(1), jnp.bfloat16(0)))
        flat = jnp.concatenate(flat, axis=1)
        for i in range(2):
            rows = slice(i * (HALF // 2), (i + 1) * (HALF // 2))
            sums[rows] += dot(flat[rows], side[0:size])

    sides = (side_0, side_1)
    messages(0, side_0)
    for tile in range(len(tiles)):
        if tile + 1 < len(tiles):
            messages(tile + 1, sides[(tile + 1) % 2])
        gather_in(tile, sides[tile % 2])
        save(tile).start()

    fresh = fresh_ref[...]
    inbound = jnp.concatenate([sums[:, :L], sums[:, L:]], axis=0).astype(BF16)
    node_in = jnp.concatenate([fresh, inbound], axis=1)
    piece = fresh.shape[0] // PIECES
    stores = []
    for i in range(PIECES):
        rows = slice(i * piece, (i + 1) * piece)
        hidden = jnp.maximum(dot(node_in[rows], nw1_ref[...]) + nb1_ref[...], 0.0).astype(BF16)
        before = dot(hidden, nw2_ref[...]) + nb2_ref[...]
        node_buf[rows] = (fresh[rows].astype(F32) + layer_norm(before, ng_ref[...], no_ref[...])).astype(BF16)
        stores.append(pltpu.make_async_copy(node_buf.at[pl.ds(i * piece, piece)], node_out.at[pl.ds(i * piece, piece)],
                                            node_sem.at[i]))
        if i:
            stores[i - 1].start()
    stores[-1].start()
    for tile in range(len(tiles)):
        save(tile).wait()
    for store in stores:
        store.wait()


VM = pl.BlockSpec(memory_space=pltpu.VMEM)
ANY = pl.BlockSpec(memory_space=pl.ANY)
HBM = pl.BlockSpec(memory_space=pltpu.HBM)


def in_hbm(x):
    return pltpu.with_memory_space_constraint(x, pltpu.HBM)


def exchange(count, old, mig_send, mig_recv, halo_send, cross_send, lines, edge_latent, vectors):
    nodes, edges = old.shape[0], edge_latent.shape[0]
    far = halo_send.shape[1] + cross_send.shape[1]
    steps = 2 * R
    kept = [((nodes, L), BF16), ((256, L), BF16), ((edges, L), F32), ((edges, L), I32),
            (lines[0].shape, I32), ((edges, L), BF16)] + [(v.shape, v.dtype) for v in vectors]
    operands = [old, mig_send, mig_recv.reshape(-1, 128), halo_send, cross_send, *lines, edge_latent, *vectors]
    params = dict(collective_id=0) if count else {}
    return pl.pallas_call(
        functools.partial(exchange_kernel, count),
        out_shape=tuple(pltpu.VMEM(shape, dtype) for shape, dtype in kept),
        in_specs=[HBM] * len(operands),
        out_specs=(VM,) * len(kept),
        scratch_shapes=[
            pltpu.VMEM(old.shape, BF16), pltpu.VMEM(mig_send.shape, I32), pltpu.VMEM((nodes // 128, 128), I32),
            pltpu.VMEM(halo_send.shape, I32), pltpu.VMEM(cross_send.shape, I32),
            pltpu.VMEM(lines[0].shape, I32), pltpu.VMEM(lines[0].shape, I32), pltpu.VMEM(lines[0].shape, I32),
            pltpu.VMEM((HALF, 2 * L), BF16), pltpu.VMEM((HALF, 2 * L), BF16),
            pltpu.VMEM((mig_send.shape[1], L), BF16), pltpu.VMEM((mig_send.shape[1], L), BF16),
            pltpu.VMEM((far, L), BF16), pltpu.VMEM((far, L), BF16),
            pltpu.VMEM((nodes, L), F32), pltpu.VMEM((nodes, mig_send.shape[1]), BF16),
            pltpu.VMEM((far, mig_send.shape[1]), BF16), pltpu.VMEM((far, L), F32),
            pltpu.VMEM((mig_send.shape[1], L), BF16), pltpu.VMEM((halo_send.shape[1], 128), BF16),
            pltpu.VMEM((halo_send.shape[1], 128), BF16),
            pltpu.VMEM((steps, 2 * L, L), BF16), pltpu.VMEM((HALF, 2 * L), BF16), pltpu.VMEM((edges, L), I32),
            pltpu.VMEM((2 * mig_send.shape[1], L), BF16),
            pltpu.SemaphoreType.DMA((9,)), pltpu.SemaphoreType.DMA((len(vectors),)),
            pltpu.SemaphoreType.DMA((steps,)), pltpu.SemaphoreType.DMA((steps,)),
            pltpu.SemaphoreType.DMA((steps + 1,)), pltpu.SemaphoreType.DMA((steps + 1,)),
            *[pltpu.SemaphoreType.DMA((steps,))] * 4,
        ],
        compiler_params=pltpu.CompilerParams(has_side_effects=True, vmem_limit_bytes=24 << 20, **params),
        name="exchange",
    )(*[in_hbm(x) for x in operands])


def layer(parts):
    nodes, edges = parts[0].shape[0], parts[2].shape[0]
    return pl.pallas_call(
        layer_kernel,
        out_shape=(pltpu.HBM((nodes, L), BF16), pltpu.HBM((edges, L), BF16)),
        in_specs=[VM] * len(parts),
        out_specs=(HBM, HBM),
        scratch_shapes=[
            pltpu.VMEM((edges, L), BF16),
            pltpu.VMEM((nodes, L), BF16),
            pltpu.VMEM((max(SIZES), 2 * L), BF16),
            pltpu.VMEM((max(SIZES), 2 * L), BF16),
            pltpu.VMEM((HALF, 2 * L), F32),
            pltpu.SemaphoreType.DMA((len(SIZES),)),
            pltpu.SemaphoreType.DMA((PIECES,)),
        ],
        compiler_params=pltpu.CompilerParams(vmem_limit_bytes=24 << 20),
        name="layer",
    )(*parts)


def step(count, node_latent, edge_latent, mig_send, mig_recv, halo_send, cross_send, senders, receivers, edge_live,
         *weights):
    vectors = [w if w.ndim == 2 else w.reshape(1, -1) for w in weights]
    lines = [v.reshape(-1, 128) for v in (senders, receivers, edge_live)]
    return layer(exchange(count, node_latent, mig_send, mig_recv, halo_send, cross_send, lines, edge_latent, vectors))


def solution(mesh):
    rows, line = P(("grp", "dom"), None), P(("grp", "dom"))
    return jax.shard_map(
        functools.partial(step, mesh.shape["dom"]),
        mesh=mesh,
        in_specs=(rows, rows, rows, line, rows, rows, line, line, line) + (P(),) * 12,
        out_specs=(rows, rows),
        check_vma=False,
    )
```
